128 devices in a mesh: gz: 16 (over z, y), gy: 8 (over x, core).
Axes of the slice: x: 4, y: 4, z: 4, core: 2. Of those that a mesh axis runs over, the one named last changes fastest.
Arguments:
- density: float32 [128, 123904], P('gz', 'gy'), may hold values from -6 to 6
Outputs:
- potential: float32 [128, 123904], P('gz', 'gy')
The draws below stay inside these ranges and needn't reach their ends.
All inputs are finite; a program needn't handle non-finite values.
Results may differ from the reference program's by a relative error of at most 0.00014.
Values sent between devices are 32-bit elements; how exact they have to be, the bound alone decides.
No kernel may reach another device: no remote copies, remote signals or barrier semaphores. Data moves between devices by JAX's collectives and lax.ppermute only.
A program may use at most 64 MiB of HBM per device.

```python
import math
import jax
import jax.numpy as jnp
from jax import lax

NX = 352
NY = 352
SCREEN = 128
NZ = 128


def block_levels(stream_key, dims, pieces, least, high):
    factor_of, own = 1.0, jax.random.fold_in(stream_key, 6)
    for position, parts in pieces:
        heights = jnp.exp(jax.random.uniform(jax.random.fold_in(own, position), (parts,), jnp.float32, least / len(pieces), high / len(pieces)))
        factor_of = factor_of * jnp.repeat(heights, dims[position] // parts).reshape([-1 if axis == position else 1 for axis in range(len(dims))])
    return factor_of


def normal_values(own_key, shape, scale, bound, split=(), held_as=jnp.bfloat16):
    array = scale * jax.random.normal(own_key, shape, jnp.float32)
    if split:
        array = array * block_levels(own_key, shape, split, -0.22, 0.18)
    return jnp.clip(array, -bound, bound).astype(held_as)


def setup_inputs(seed: int = 0) -> dict:
    keys = jax.random.split(jax.random.key(seed), 2)
    return {
        "density": normal_values(keys[0], (NZ, NY * NX), 1.0, 6.0, ((0, 16), (1, 8)), jnp.float32),
    }


def reference(density):
    planes = density.shape[0]
    width_x = NX
    width_y = NY
    field = jnp.transpose(density.reshape(planes, width_y, width_x), (0, 2, 1))
    hat = jnp.fft.rfft2(field, axes=(1, 2))
    index_x = jnp.arange(width_x, dtype=jnp.int32)
    wave_x = jnp.minimum(index_x, width_x - index_x).astype(jnp.float32) * (2.0 * math.pi / width_x)
    wave_y = jnp.arange(width_y // 2 + 1, dtype=jnp.int32).astype(jnp.float32) * (2.0 * math.pi / width_y)
    kappa = jnp.sqrt(1.0 / (SCREEN * SCREEN) + wave_x[:, None] ** 2 + wave_y[None, :] ** 2)
    decay = jnp.exp(-kappa)

    def forward(carry, plane):
        carry = decay * carry + plane
        return (carry, carry)

    def backward(carry, plane):
        return (decay * (carry + plane), carry)
    _, upward = lax.scan(forward, jnp.zeros_like(hat[0]), hat)
    _, downward = lax.scan(backward, jnp.zeros_like(hat[0]), hat, reverse=True)
    phi = (upward + downward) * (0.5 / kappa)
    result = jnp.fft.irfft2(phi, s=(width_x, width_y), axes=(1, 2)).astype(jnp.float32)
    return jnp.transpose(result, (0, 2, 1)).reshape(planes, width_y * width_x)
```

```python
import math

import jax
import jax.numpy as jnp
import numpy as np
from jax import lax
from jax.experimental import pallas as pl
from jax.experimental.pallas import tpu as pltpu
from jax.sharding import PartitionSpec as P

NX = 352
NY = 352
SCREEN = 128
TWO_PI = 2.0 * math.pi

PAD = 384
LANES = 128
TILES = PAD // LANES
GZ = 16
GY = 8
PLANES = 8
ROWS = NY // GY
CHUNK = PAD // GY
OWN = 3
PEERS = GZ * GY
SEND = PEERS * OWN * TILES
BELONG = OWN * TILES

F32 = jnp.float32
BF16 = jnp.bfloat16


def real_basis(length):
    index = np.arange(length)
    basis = np.zeros((length, length))
    for row in range(length):
        m = (row + 1) // 2
        angle = 2.0 * np.pi * ((m * index) % length) / length
        wave = np.cos(angle) if row % 2 == 1 or row == 0 else np.sin(angle)
        weight = 1.0 if row == 0 or row == length - 1 else 2.0
        basis[row] = wave * np.sqrt(weight / length)
    return basis


def halves(table):
    single = table.astype(np.float32)
    high = single.astype(jnp.bfloat16)
    low = (single - high.astype(np.float32)).astype(jnp.bfloat16)
    return high, low


def x_table():
    table = np.zeros((PAD, PAD))
    table[:NX, :NX] = real_basis(NX)
    return halves(table)


def y_table():
    table = np.zeros((PAD, GY, CHUNK))
    table[:NY, :, :ROWS] = real_basis(NY).reshape(NY, GY, ROWS)
    return halves(table.reshape(PAD, PAD))


def split(value):
    high = value.astype(BF16)
    return high, (value - high.astype(F32)).astype(BF16)


def product(left, right, dims):
    def dot(a, b):
        return lax.dot_general(a, b, (dims, ((), ())), preferred_element_type=F32)

    return dot(left[0], right[0]) + (dot(left[0], right[1]) + dot(left[1], right[0]))


def lane_tile(j):
    return slice(j * LANES, (j + 1) * LANES)


def forward_x(x_ref, high_ref, low_ref, out_ref, field_ref):
    for y in range(CHUNK):
        if y < ROWS:
            offset = y * NX
            shift = offset % LANES
            width = PAD if shift <= PAD - NX else PAD + LANES
            value = x_ref[:, pl.ds(offset - shift, width)]
            if shift:
                value = pltpu.roll(value, width - shift, 1)
        else:
            value = jnp.zeros((PLANES, PAD), F32)
        for j in range(TILES):
            field_ref[j, pl.ds(y, PLANES, stride=CHUNK), :] = value[:, lane_tile(j)]
    field = jnp.concatenate([field_ref[j] for j in range(TILES)], axis=1)
    result = product((high_ref[...], low_ref[...]), split(field), ((1,), (1,)))
    for j in range(TILES):
        out_ref[pl.ds(j, PAD, stride=TILES), :] = result[:, lane_tile(j)]


def chunk_pick(parts, lane):
    out = []
    for j in range(TILES):
        first = j * LANES // CHUNK
        last = ((j + 1) * LANES - 1) // CHUNK
        value = parts[last][j]
        for c in range(last - 1, first - 1, -1):
            value = jnp.where(lane < (c + 1) * CHUNK - j * LANES, parts[c][j], value)
        out.append(value)
    return out


def swap_chunks(arrays, lane):
    turned = []
    for d in range(GY):
        picked = chunk_pick([arrays[(c + d) % GY] for c in range(GY)], lane)
        whole = jnp.concatenate(picked, axis=1)
        if d:
            whole = pltpu.roll(whole, CHUNK * d, 1)
        turned.append([whole[:, lane_tile(j)] for j in range(TILES)])
    return [chunk_pick([turned[(c - b) % GY] for c in range(GY)], lane) for b in range(GY)]


def middle(in_ref, high_ref, low_ref, decay_ref, scale_ref, out_ref, work_ref, phi_ref):
    lane = lax.broadcasted_iota(jnp.int32, (8, LANES), 1)
    block = OWN * GZ
    for tile in range(block // 8):
        own, half = divmod(tile, GZ // 8)
        arrays = [
            [
                in_ref[pl.ds((half * 8 * GY + g) * BELONG + own * TILES + j, 8, stride=GY * BELONG), :]
                for j in range(TILES)
            ]
            for g in range(GY)
        ]
        for z, parts in enumerate(swap_chunks(arrays, lane)):
            for j in range(TILES):
                work_ref[pl.ds(z * block + tile * 8, 8), lane_tile(j)] = parts[j]
    table = (high_ref[...], low_ref[...])
    phi_ref[...] = product(split(work_ref[...]), table, ((1,), (1,)))

    gz = lax.broadcasted_iota(jnp.int32, (GZ, LANES), 0)
    for own in range(OWN):
        for j in range(TILES):
            decay = decay_ref[pl.ds(own, 1), lane_tile(j)]
            scale = scale_ref[pl.ds(own, 1), lane_tile(j)]
            decay = jnp.broadcast_to(decay, (GZ, LANES))
            scale = jnp.broadcast_to(scale, (GZ, LANES))
            hat = [phi_ref[pl.ds(z * block + own * GZ, GZ), lane_tile(j)] for z in range(PLANES)]
            up = [hat[0]]
            for z in range(1, PLANES):
                up.append(decay * up[-1] + hat[z])
            down = [jnp.zeros((GZ, LANES), F32)]
            for z in range(PLANES - 1, 0, -1):
                down.append(decay * (down[-1] + hat[z]))
            down = down[::-1]
            over = up[-1]
            under = decay * (down[0] + hat[0])
            power = decay * decay
            power = power * power
            power = power * power
            step = 1
            while step < GZ:
                over = over + jnp.where(gz >= step, power * pltpu.roll(over, step, 0), 0.0)
                under = under + jnp.where(gz < GZ - step, power * pltpu.roll(under, GZ - step, 0), 0.0)
                power = power * power
                step *= 2
            over = jnp.where(gz >= 1, pltpu.roll(over, 1, 0), 0.0)
            under = jnp.where(gz < GZ - 1, pltpu.roll(under, GZ - 1, 0), 0.0)
            for z in range(PLANES):
                over = decay * over
                up[z] = up[z] + over
            for z in range(PLANES - 1, -1, -1):
                down[z] = down[z] + under
                under = decay * under
            for z in range(PLANES):
                phi_ref[pl.ds(z * block + own * GZ, GZ), lane_tile(j)] = (up[z] + down[z]) * scale

    work_ref[...] = product(split(phi_ref[...]), table, ((1,), (0,)))
    for tile in range(block // 8):
        own, half = divmod(tile, GZ // 8)
        arrays = [
            [work_ref[pl.ds(z * block + tile * 8, 8), lane_tile(j)] for j in range(TILES)] for z in range(PLANES)
        ]
        for g, parts in enumerate(swap_chunks(arrays, lane)):
            for j in range(TILES):
                out_ref[pl.ds((half * 8 * GY + g) * BELONG + own * TILES + j, 8, stride=GY * BELONG), :] = parts[j]


def backward_x(in_ref, high_ref, low_ref, out_ref, field_ref):
    value = jnp.concatenate([in_ref[pl.ds(j, PAD, stride=TILES), :] for j in range(TILES)], axis=1)
    table = (high_ref[...], low_ref[...])
    result = product(split(jnp.transpose(value)), table, ((1,), (0,)))
    for j in range(TILES):
        field_ref[j] = result[:, lane_tile(j)]
    carry = None
    for y in range(ROWS):
        offset = y * NX
        shift = offset % LANES
        value = jnp.concatenate([field_ref[j, pl.ds(y, PLANES, stride=CHUNK), :] for j in range(TILES)], axis=1)
        if shift > PAD - NX:
            value = jnp.concatenate([value, jnp.zeros((PLANES, LANES), F32)], axis=1)
        if shift:
            value = pltpu.roll(value, shift, 1)
        tiles = [value[:, lane_tile(j)] for j in range(value.shape[1] // LANES)]
        if carry is not None:
            tiles[0] = tiles[0] + carry
        end = shift + NX
        full = end // LANES
        carry = tiles[full] if end % LANES else None
        for j in range(full):
            out_ref[:, pl.ds(offset - shift + j * LANES, LANES)] = tiles[j]


def call(kernel, out_shape, scratch, *args):
    return pl.pallas_call(
        kernel,
        out_shape=jax.ShapeDtypeStruct(out_shape, F32),
        in_specs=[pl.BlockSpec(memory_space=pltpu.VMEM)] * len(args),
        out_specs=pl.BlockSpec(memory_space=pltpu.VMEM),
        scratch_shapes=[pltpu.VMEM(shape, F32) for shape in scratch],
    )(*args)


def wavenumber(index, length):
    return ((index + 1) // 2).astype(F32) * (TWO_PI / length)


def exchange(buffer):
    return lax.all_to_all(buffer, ("gz", "gy"), 0, 0, tiled=True)


def on_device(density):
    x_high, x_low = (jnp.asarray(t) for t in x_table())
    y_high, y_low = (jnp.asarray(t) for t in y_table())
    own = lax.axis_index("gz") * GY + lax.axis_index("gy")
    index_x = jnp.minimum(own * OWN + jnp.arange(OWN, dtype=jnp.int32), NX - 1)
    index_y = jnp.minimum(jnp.arange(PAD, dtype=jnp.int32), NY - 1)
    wave_x = wavenumber(index_x, NX)
    wave_y = wavenumber(index_y, NY)
    kappa = jnp.sqrt(1.0 / (SCREEN * SCREEN) + wave_x[:, None] ** 2 + wave_y[None, :] ** 2)
    decay = jnp.exp(-kappa)
    scale = 0.5 / kappa

    field = [(TILES, PAD, LANES)]
    sent = call(forward_x, (SEND, LANES), field, density, x_high, x_low)
    held = exchange(sent)
    back = call(middle, (SEND, LANES), [(PAD, PAD)] * 2, held, y_high, y_low, decay, scale)
    held = exchange(back)
    return call(backward_x, density.shape, field, held, x_high, x_low)


def solution(mesh):
    return jax.shard_map(
        on_device,
        mesh=mesh,
        in_specs=(P("gz", "gy"),),
        out_specs=P("gz", "gy"),
        check_vma=False,
    )
```

```python
import math

import jax
import jax.numpy as jnp
import numpy as np
from jax import lax
from jax.experimental import pallas as pl
from jax.experimental.pallas import tpu as pltpu
from jax.sharding import PartitionSpec as P

NX = 352
NY = 352
SCREEN = 128
TWO_PI = 2.0 * math.pi

PAD = 384
LANES = 128
TILES = PAD // LANES
GZ = 16
GY = 8
PLANES = 8
ROWS = NY // GY
CHUNK = PAD // GY
OWN = 3
PEERS = GZ * GY
SEND = PEERS * OWN * TILES
BELONG = OWN * TILES

F32 = jnp.float32
BF16 = jnp.bfloat16


def real_basis(length):
    index = np.arange(length)
    basis = np.zeros((length, length))
    for row in range(length):
        m = (row + 1) // 2
        angle = 2.0 * np.pi * ((m * index) % length) / length
        wave = np.cos(angle) if row % 2 == 1 or row == 0 else np.sin(angle)
        weight = 1.0 if row == 0 or row == length - 1 else 2.0
        basis[row] = wave * np.sqrt(weight / length)
    return basis


def halves(table):
    single = table.astype(np.float32)
    high = single.astype(jnp.bfloat16)
    low = (single - high.astype(np.float32)).astype(jnp.bfloat16)
    return high, low


def x_table():
    table = np.zeros((PAD, PAD))
    table[:NX, :NX] = real_basis(NX)
    return halves(table)


def y_table():
    table = np.zeros((PAD, GY, CHUNK))
    table[:NY, :, :ROWS] = real_basis(NY).reshape(NY, GY, ROWS)
    return halves(table.reshape(PAD, PAD))


def split(value):
    high = value.astype(BF16)
    return high, (value - high.astype(F32)).astype(BF16)


def product(left, right, dims):
    def dot(a, b):
        return lax.dot_general(a, b, (dims, ((), ())), preferred_element_type=F32)

    return dot(left[0], right[0]) + (dot(left[0], right[1]) + dot(left[1], right[0]))


def lane_tile(j):
    return slice(j * LANES, (j + 1) * LANES)


def forward_x(x_ref, high_ref, low_ref, out_ref, field_ref):
    for y in range(CHUNK):
        if y < ROWS:
            offset = y * NX
            shift = offset % LANES
            width = PAD if shift <= PAD - NX else PAD + LANES
            value = x_ref[:, pl.ds(offset - shift, width)]
            if shift:
                value = pltpu.roll(value, width - shift, 1)
        else:
            value = jnp.zeros((PLANES, PAD), F32)
        for j in range(TILES):
            field_ref[j, pl.ds(y, PLANES, stride=CHUNK), :] = value[:, lane_tile(j)]
    field = jnp.concatenate([field_ref[j] for j in range(TILES)], axis=1)
    result = product((high_ref[...], low_ref[...]), split(field), ((1,), (1,)))
    for j in range(TILES):
        out_ref[pl.ds(j, PAD, stride=TILES), :] = result[:, lane_tile(j)]


def chunk_pick(parts, lane):
    out = []
    for j in range(TILES):
        first = j * LANES // CHUNK
        last = ((j + 1) * LANES - 1) // CHUNK
        value = parts[last][j]
        for c in range(last - 1, first - 1, -1):
            value = jnp.where(lane < (c + 1) * CHUNK - j * LANES, parts[c][j], value)
        out.append(value)
    return out


def swap_chunks(arrays, lane):
    turned = []
    for d in range(GY):
        picked = chunk_pick([arrays[(c + d) % GY] for c in range(GY)], lane)
        whole = jnp.concatenate(picked, axis=1)
        if d:
            whole = pltpu.roll(whole, CHUNK * d, 1)
        turned.append([whole[:, lane_tile(j)] for j in range(TILES)])
    return [chunk_pick([turned[(c - b) % GY] for c in range(GY)], lane) for b in range(GY)]


def middle(in_ref, high_ref, low_ref, decay_ref, scale_ref, out_ref, work_ref, phi_ref):
    lane = lax.broadcasted_iota(jnp.int32, (8, LANES), 1)
    block = OWN * GZ
    for tile in range(block // 8):
        own, half = divmod(tile, GZ // 8)
        arrays = [
            [
                in_ref[pl.ds((half * 8 * GY + g) * BELONG + own * TILES + j, 8, stride=GY * BELONG), :]
                for j in range(TILES)
            ]
            for g in range(GY)
        ]
        for z, parts in enumerate(swap_chunks(arrays, lane)):
            for j in range(TILES):
                work_ref[pl.ds(z * block + tile * 8, 8), lane_tile(j)] = parts[j]
    table = (high_ref[...], low_ref[...])
    phi_ref[...] = product(split(work_ref[...]), table, ((1,), (1,)))

    gz = lax.broadcasted_iota(jnp.int32, (GZ, LANES), 0)
    for own in range(OWN):
        for j in range(TILES):
            decay = decay_ref[pl.ds(own, 1), lane_tile(j)]
            scale = scale_ref[pl.ds(own, 1), lane_tile(j)]
            decay = jnp.broadcast_to(decay, (GZ, LANES))
            scale = jnp.broadcast_to(scale, (GZ, LANES))
            hat = [phi_ref[pl.ds(z * block + own * GZ, GZ), lane_tile(j)] for z in range(PLANES)]
            up = [hat[0]]
            for z in range(1, PLANES):
                up.append(decay * up[-1] + hat[z])
            down = [jnp.zeros((GZ, LANES), F32)]
            for z in range(PLANES - 1, 0, -1):
                down.append(decay * (down[-1] + hat[z]))
            down = down[::-1]
            over = up[-1]
            under = decay * (down[0] + hat[0])
            power = decay * decay
            power = power * power
            power = power * power
            step = 1
            while step < GZ:
                over = over + jnp.where(gz >= step, power * pltpu.roll(over, step, 0), 0.0)
                under = under + jnp.where(gz < GZ - step, power * pltpu.roll(under, GZ - step, 0), 0.0)
                power = power * power
                step *= 2
            over = jnp.where(gz >= 1, pltpu.roll(over, 1, 0), 0.0)
            under = jnp.where(gz < GZ - 1, pltpu.roll(under, GZ - 1, 0), 0.0)
            for z in range(PLANES):
                over = decay * over
                up[z] = up[z] + over
            for z in range(PLANES - 1, -1, -1):
                down[z] = down[z] + under
                under = decay * under
            for z in range(PLANES):
                phi_ref[pl.ds(z * block + own * GZ, GZ), lane_tile(j)] = (up[z] + down[z]) * scale

    work_ref[...] = product(split(phi_ref[...]), table, ((1,), (0,)))
    for tile in range(block // 8):
        own, half = divmod(tile, GZ // 8)
        arrays = [
            [work_ref[pl.ds(z * block + tile * 8, 8), lane_tile(j)] for j in range(TILES)] for z in range(PLANES)
        ]
        for g, parts in enumerate(swap_chunks(arrays, lane)):
            for j in range(TILES):
                out_ref[pl.ds((half * 8 * GY + g) * BELONG + own * TILES + j, 8, stride=GY * BELONG), :] = parts[j]


def backward_x(in_ref, high_ref, low_ref, out_ref, field_ref):
    value = jnp.concatenate([in_ref[pl.ds(j, PAD, stride=TILES), :] for j in range(TILES)], axis=1)
    table = (high_ref[...], low_ref[...])
    result = product(split(jnp.transpose(value)), table, ((1,), (0,)))
    for j in range(TILES):
        field_ref[j] = result[:, lane_tile(j)]
    carry = None
    for y in range(ROWS):
        offset = y * NX
        shift = offset % LANES
        value = jnp.concatenate([field_ref[j, pl.ds(y, PLANES, stride=CHUNK), :] for j in range(TILES)], axis=1)
        if shift > PAD - NX:
            value = jnp.concatenate([value, jnp.zeros((PLANES, LANES), F32)], axis=1)
        if shift:
            value = pltpu.roll(value, shift, 1)
        tiles = [value[:, lane_tile(j)] for j in range(value.shape[1] // LANES)]
        if carry is not None:
            tiles[0] = tiles[0] + carry
        end = shift + NX
        full = end // LANES
        carry = tiles[full] if end % LANES else None
        for j in range(full):
            out_ref[:, pl.ds(offset - shift + j * LANES, LANES)] = tiles[j]


def call(kernel, out_shape, scratch, *args):
    return pl.pallas_call(
        kernel,
        out_shape=jax.ShapeDtypeStruct(out_shape, F32),
        in_specs=[pl.BlockSpec(memory_space=pltpu.VMEM)] * len(args),
        out_specs=pl.BlockSpec(memory_space=pltpu.VMEM),
        scratch_shapes=[pltpu.VMEM(shape, F32) for shape in scratch],
    )(*args)


def wavenumber(index, length):
    return ((index + 1) // 2).astype(F32) * (TWO_PI / length)


def exchange(buffer):
    whole = buffer.reshape(PEERS, 1, BELONG * LANES)
    whole = lax.all_to_all(whole, ("gz", "gy"), 0, 0, tiled=True)
    return whole.reshape(SEND, LANES)


def on_device(density):
    x_high, x_low = (jnp.asarray(t) for t in x_table())
    y_high, y_low = (jnp.asarray(t) for t in y_table())
    own = lax.axis_index("gz") * GY + lax.axis_index("gy")
    index_x = jnp.minimum(own * OWN + jnp.arange(OWN, dtype=jnp.int32), NX - 1)
    index_y = jnp.minimum(jnp.arange(PAD, dtype=jnp.int32), NY - 1)
    wave_x = wavenumber(index_x, NX)
    wave_y = wavenumber(index_y, NY)
    kappa = jnp.sqrt(1.0 / (SCREEN * SCREEN) + wave_x[:, None] ** 2 + wave_y[None, :] ** 2)
    decay = jnp.exp(-kappa)
    scale = 0.5 / kappa

    field = [(TILES, PAD, LANES)]
    sent = call(forward_x, (SEND, LANES), field, density, x_high, x_low)
    held = exchange(sent)
    back = call(middle, (SEND, LANES), [(PAD, PAD)] * 2, held, y_high, y_low, decay, scale)
    held = exchange(back)
    return call(backward_x, density.shape, field, held, x_high, x_low)


def solution(mesh):
    return jax.shard_map(
        on_device,
        mesh=mesh,
        in_specs=(P("gz", "gy"),),
        out_specs=P("gz", "gy"),
        check_vma=False,
    )
```

```python
import math

import jax
import jax.numpy as jnp
import numpy as np
from jax import lax
from jax.experimental import pallas as pl
from jax.experimental.pallas import tpu as pltpu
from jax.sharding import PartitionSpec as P

NX = 352
NY = 352
SCREEN = 128
TWO_PI = 2.0 * math.pi

PAD = 384
LANES = 128
TILES = PAD // LANES
GZ = 16
GY = 8
PLANES = 8
ROWS = NY // GY
CHUNK = PAD // GY
OWN = 3
PEERS = GZ * GY
SEND = PEERS * OWN * TILES
BELONG = OWN * TILES

F32 = jnp.float32
BF16 = jnp.bfloat16


def real_basis(length):
    index = np.arange(length)
    basis = np.zeros((length, length))
    for row in range(length):
        m = (row + 1) // 2
        angle = 2.0 * np.pi * ((m * index) % length) / length
        wave = np.cos(angle) if row % 2 == 1 or row == 0 else np.sin(angle)
        weight = 1.0 if row == 0 or row == length - 1 else 2.0
        basis[row] = wave * np.sqrt(weight / length)
    return basis


def halves(table):
    single = table.astype(np.float32)
    high = single.astype(jnp.bfloat16)
    low = (single - high.astype(np.float32)).astype(jnp.bfloat16)
    return high, low


def x_table():
    table = np.zeros((PAD, PAD))
    table[:NX, :NX] = real_basis(NX)
    return halves(table)


def y_table():
    table = np.zeros((PAD, GY, CHUNK))
    table[:NY, :, :ROWS] = real_basis(NY).reshape(NY, GY, ROWS)
    return halves(table.reshape(PAD, PAD))


def split(value):
    high = value.astype(BF16)
    return high, (value - high.astype(F32)).astype(BF16)


def product(left, right, dims):
    def dot(a, b):
        return lax.dot_general(a, b, (dims, ((), ())), preferred_element_type=F32)

    return dot(left[0], right[0]) + (dot(left[0], right[1]) + dot(left[1], right[0]))


def lane_tile(j):
    return slice(j * LANES, (j + 1) * LANES)


def forward_x(x_ref, high_ref, low_ref, out_ref, field_ref):
    for y in range(CHUNK):
        if y < ROWS:
            offset = y * NX
            shift = offset % LANES
            width = PAD if shift <= PAD - NX else PAD + LANES
            value = x_ref[:, pl.ds(offset - shift, width)]
            if shift:
                value = pltpu.roll(value, width - shift, 1)
        else:
            value = jnp.zeros((PLANES, PAD), F32)
        for j in range(TILES):
            field_ref[j, pl.ds(y, PLANES, stride=CHUNK), :] = value[:, lane_tile(j)]
    field = jnp.concatenate([field_ref[j] for j in range(TILES)], axis=1)
    result = product((high_ref[...], low_ref[...]), split(field), ((1,), (1,)))
    for j in range(TILES):
        out_ref[pl.ds(j, PAD, stride=TILES), :] = result[:, lane_tile(j)]


def chunk_pick(parts, lane):
    out = []
    for j in range(TILES):
        first = j * LANES // CHUNK
        last = ((j + 1) * LANES - 1) // CHUNK
        value = parts[last][j]
        for c in range(last - 1, first - 1, -1):
            value = jnp.where(lane < (c + 1) * CHUNK - j * LANES, parts[c][j], value)
        out.append(value)
    return out


def swap_chunks(arrays, lane):
    turned = []
    for d in range(GY):
        picked = chunk_pick([arrays[(c + d) % GY] for c in range(GY)], lane)
        whole = jnp.concatenate(picked, axis=1)
        if d:
            whole = pltpu.roll(whole, CHUNK * d, 1)
        turned.append([whole[:, lane_tile(j)] for j in range(TILES)])
    return [chunk_pick([turned[(c - b) % GY] for c in range(GY)], lane) for b in range(GY)]


def kappa_tile(own, j):
    device = lax.axis_index("gz") * GY + lax.axis_index("gy")
    index_x = jnp.minimum(device * OWN + own, NX - 1)
    lane = lax.broadcasted_iota(jnp.int32, (GZ, LANES), 1)
    index_y = jnp.minimum(lane + j * LANES, NY - 1)
    wave_x = jnp.full((GZ, LANES), lax.shift_right_logical(index_x + 1, 1), jnp.int32).astype(F32) * (TWO_PI / NX)
    wave_y = lax.shift_right_logical(index_y + 1, 1).astype(F32) * (TWO_PI / NY)
    return jnp.sqrt(1.0 / (SCREEN * SCREEN) + wave_x * wave_x + wave_y * wave_y)


def middle(in_ref, high_ref, low_ref, out_ref, work_ref, phi_ref):
    lane = lax.broadcasted_iota(jnp.int32, (8, LANES), 1)
    block = OWN * GZ
    for tile in range(block // 8):
        own, half = divmod(tile, GZ // 8)
        arrays = [
            [
                in_ref[pl.ds((half * 8 * GY + g) * BELONG + own * TILES + j, 8, stride=GY * BELONG), :]
                for j in range(TILES)
            ]
            for g in range(GY)
        ]
        for z, parts in enumerate(swap_chunks(arrays, lane)):
            for j in range(TILES):
                work_ref[pl.ds(z * block + tile * 8, 8), lane_tile(j)] = parts[j]
    table = (high_ref[...], low_ref[...])
    phi_ref[...] = product(split(work_ref[...]), table, ((1,), (1,)))

    gz = lax.broadcasted_iota(jnp.int32, (GZ, LANES), 0)
    for own in range(OWN):
        for j in range(TILES):
            kappa = kappa_tile(own, j)
            decay = jnp.exp(-kappa)
            scale = 0.5 / kappa
            hat = [phi_ref[pl.ds(z * block + own * GZ, GZ), lane_tile(j)] for z in range(PLANES)]
            up = [hat[0]]
            for z in range(1, PLANES):
                up.append(decay * up[-1] + hat[z])
            down = [jnp.zeros((GZ, LANES), F32)]
            for z in range(PLANES - 1, 0, -1):
                down.append(decay * (down[-1] + hat[z]))
            down = down[::-1]
            over = up[-1]
            under = decay * (down[0] + hat[0])
            power = decay * decay
            power = power * power
            power = power * power
            step = 1
            while step < GZ:
                over = over + jnp.where(gz >= step, power * pltpu.roll(over, step, 0), 0.0)
                under = under + jnp.where(gz < GZ - step, power * pltpu.roll(under, GZ - step, 0), 0.0)
                power = power * power
                step *= 2
            over = jnp.where(gz >= 1, pltpu.roll(over, 1, 0), 0.0)
            under = jnp.where(gz < GZ - 1, pltpu.roll(under, GZ - 1, 0), 0.0)
            for z in range(PLANES):
                over = decay * over
                up[z] = up[z] + over
            for z in range(PLANES - 1, -1, -1):
                down[z] = down[z] + under
                under = decay * under
            for z in range(PLANES):
                phi_ref[pl.ds(z * block + own * GZ, GZ), lane_tile(j)] = (up[z] + down[z]) * scale

    work_ref[...] = product(split(phi_ref[...]), table, ((1,), (0,)))
    for tile in range(block // 8):
        own, half = divmod(tile, GZ // 8)
        arrays = [
            [work_ref[pl.ds(z * block + tile * 8, 8), lane_tile(j)] for j in range(TILES)] for z in range(PLANES)
        ]
        for g, parts in enumerate(swap_chunks(arrays, lane)):
            for j in range(TILES):
                out_ref[pl.ds((half * 8 * GY + g) * BELONG + own * TILES + j, 8, stride=GY * BELONG), :] = parts[j]


def backward_x(in_ref, high_ref, low_ref, out_ref, field_ref):
    value = jnp.concatenate([in_ref[pl.ds(j, PAD, stride=TILES), :] for j in range(TILES)], axis=1)
    table = (high_ref[...], low_ref[...])
    result = product(split(jnp.transpose(value)), table, ((1,), (0,)))
    for j in range(TILES):
        field_ref[j] = result[:, lane_tile(j)]
    carry = None
    for y in range(ROWS):
        offset = y * NX
        shift = offset % LANES
        value = jnp.concatenate([field_ref[j, pl.ds(y, PLANES, stride=CHUNK), :] for j in range(TILES)], axis=1)
        if shift > PAD - NX:
            value = jnp.concatenate([value, jnp.zeros((PLANES, LANES), F32)], axis=1)
        if shift:
            value = pltpu.roll(value, shift, 1)
        tiles = [value[:, lane_tile(j)] for j in range(value.shape[1] // LANES)]
        if carry is not None:
            tiles[0] = tiles[0] + carry
        end = shift + NX
        full = end // LANES
        carry = tiles[full] if end % LANES else None
        for j in range(full):
            out_ref[:, pl.ds(offset - shift + j * LANES, LANES)] = tiles[j]


def call(kernel, out_shape, scratch, *args):
    return pl.pallas_call(
        kernel,
        out_shape=out_shape,
        in_specs=[pl.BlockSpec(memory_space=pltpu.VMEM)] * len(args),
        out_specs=pl.BlockSpec(memory_space=pltpu.VMEM),
        scratch_shapes=[pltpu.VMEM(shape, F32) for shape in scratch],
    )(*(pltpu.with_memory_space_constraint(a, pltpu.VMEM) for a in args))


def exchange(buffer):
    whole = buffer.reshape(PEERS, 1, BELONG * LANES)
    whole = lax.all_to_all(whole, ("gz", "gy"), 0, 0, tiled=True)
    return whole.reshape(SEND, LANES)


def on_device(density):
    x_high, x_low = (jnp.asarray(t) for t in x_table())
    y_high, y_low = (jnp.asarray(t) for t in y_table())
    field = [(TILES, PAD, LANES)]
    sent = call(forward_x, pltpu.VMEM((SEND, LANES), F32), field, density, x_high, x_low)
    held = exchange(sent)
    back = call(middle, pltpu.VMEM((SEND, LANES), F32), [(PAD, PAD)] * 2, held, y_high, y_low)
    held = exchange(back)
    return call(backward_x, jax.ShapeDtypeStruct(density.shape, F32), field, held, x_high, x_low)


def solution(mesh):
    return jax.shard_map(
        on_device,
        mesh=mesh,
        in_specs=(P("gz", "gy"),),
        out_specs=P("gz", "gy"),
        check_vma=False,
    )
```

```python
import math

import jax
import jax.numpy as jnp
import numpy as np
from jax import lax
from jax.experimental import pallas as pl
from jax.experimental.pallas import tpu as pltpu
from jax.sharding import PartitionSpec as P

NX = 352
NY = 352
SCREEN = 128
TWO_PI = 2.0 * math.pi

PAD = 384
LANES = 128
TILES = PAD // LANES
HALF = NX // 2
SLOT = PAD // 2
PAIR = 2 * LANES
GZ = 16
GY = 8
PLANES = 8
ROWS = NY // GY
CHUNK = PAD // GY
GROUP = 8 * HALF
OWN = 3
PEERS = GZ * GY
SEND = PEERS * OWN * TILES
BELONG = OWN * TILES

F32 = jnp.float32
BF16 = jnp.bfloat16


def component(parity, row):
    return 2 * ((row + 1 - parity) >> 1) + parity


def half_basis(length):
    half = length // 2
    index = np.arange(half)
    basis = np.zeros((2, half, half))
    for parity in range(2):
        for row in range(half):
            m = component(parity, row)
            angle = 2.0 * np.pi * ((m * index) % length) / length
            cosine = row == 0 or (row + parity) % 2 == 1 or m == half
            if parity == 1:
                cosine = row % 2 == 0
            weight = 1.0 if m in (0, half) else 2.0
            basis[parity, row] = (np.cos(angle) if cosine else np.sin(angle)) * np.sqrt(weight / length)
    return basis


def halves(table):
    single = table.astype(np.float32)
    high = single.astype(jnp.bfloat16)
    low = (single - high.astype(np.float32)).astype(jnp.bfloat16)
    return np.stack([high, low])


def x_table():
    table = np.zeros((2, SLOT, PAIR))
    table[:, :HALF, :HALF] = half_basis(NX)
    return halves(table)


def y_table():
    block = np.zeros((2, SLOT, GY // 2, CHUNK))
    block[:, :HALF, :, :ROWS] = half_basis(NY).reshape(2, HALF, GY // 2, ROWS)
    block = block.reshape(2, SLOT, SLOT)
    table = np.zeros((2, PAIR, PAIR))
    table[0, :SLOT, :SLOT] = block[0]
    table[1, PAIR - SLOT :, PAIR - SLOT :] = block[1]
    return halves(table)


def split(value):
    high = value.astype(BF16)
    return high, (value - high.astype(F32)).astype(BF16)


def product(left, right, dims):
    def dot(a, b):
        return lax.dot_general(a, b, (dims, ((), ())), preferred_element_type=F32)

    return dot(left[0], right[0]) + (dot(left[0], right[1]) + dot(left[1], right[0]))


def lane_tile(j):
    return slice(j * LANES, (j + 1) * LANES)


def table_of(table_ref, parity):
    return table_ref[0, parity], table_ref[1, parity]


def half_row(ref, offset):
    shift = offset % LANES
    width = -(-(shift + HALF) // LANES) * LANES
    value = ref[:, pl.ds(offset - shift, width)]
    if shift:
        value = pltpu.roll(value, width - shift, 1)
    return value[:, :PAIR]


def forward_x(x_ref, table_ref, out_ref, field_ref, flat_ref, local_ref, x_sems, table_sem):
    loads = []
    for n in range(NX * ROWS // GROUP):
        part = pl.ds(n * GROUP, GROUP)
        loads.append(pltpu.make_async_copy(x_ref.at[:, part], flat_ref.at[:, part], x_sems.at[n]))
    table_load = pltpu.make_async_copy(table_ref, local_ref, table_sem)
    for load in loads:
        load.start()
    table_load.start()
    for y in range(ROWS, CHUNK):
        for j in range(4):
            field_ref[j, pl.ds(y, PLANES, stride=CHUNK), :] = jnp.zeros((PLANES, LANES), F32)
    for n, load in enumerate(loads):
        load.wait()
        for y in range(n * GROUP // NX, (n + 1) * GROUP // NX):
            one = half_row(flat_ref, y * NX)
            two = half_row(flat_ref, y * NX + HALF)
            for parity, value in enumerate((one + two, one - two)):
                for j in range(2):
                    field_ref[2 * parity + j, pl.ds(y, PLANES, stride=CHUNK), :] = value[:, lane_tile(j)]
    table_load.wait()
    for parity in range(2):
        field = jnp.concatenate([field_ref[2 * parity + j] for j in range(2)], axis=1)
        result = product(table_of(local_ref, parity), split(field), ((1,), (1,)))
        for j in range(TILES):
            out_ref[pl.ds(parity * SLOT * TILES + j, SLOT, stride=TILES), :] = result[:, lane_tile(j)]


def chunk_pick(parts, lane):
    out = []
    for j in range(TILES):
        first = j * LANES // CHUNK
        last = ((j + 1) * LANES - 1) // CHUNK
        value = parts[last][j]
        for c in range(last - 1, first - 1, -1):
            value = jnp.where(lane < (c + 1) * CHUNK - j * LANES, parts[c][j], value)
        out.append(value)
    return out


def swap_chunks(arrays, lane):
    turned = []
    for d in range(GY):
        picked = chunk_pick([arrays[(c + d) % GY] for c in range(GY)], lane)
        whole = jnp.concatenate(picked, axis=1)
        if d:
            whole = pltpu.roll(whole, CHUNK * d, 1)
        turned.append([whole[:, lane_tile(j)] for j in range(TILES)])
    return [chunk_pick([turned[(c - b) % GY] for c in range(GY)], lane) for b in range(GY)]


def butterfly(arrays):
    pairs = [list(zip(arrays[g], arrays[g + GY // 2])) for g in range(GY // 2)]
    return [[a + b for a, b in p] for p in pairs] + [[a - b for a, b in p] for p in pairs]


def both_parities(value_ref, table_ref, dims, out_ref):
    even = product(split(value_ref[:, :PAIR]), table_of(table_ref, 0), dims)
    odd = product(split(value_ref[:, PAD - PAIR :]), table_of(table_ref, 1), dims)
    out_ref[:, lane_tile(0)] = even[:, :LANES]
    out_ref[:, lane_tile(1)] = even[:, LANES:] + odd[:, :LANES]
    out_ref[:, lane_tile(2)] = odd[:, LANES:]


def wavenumber(index, length):
    parity = (index >= SLOT).astype(jnp.int32)
    row = jnp.minimum(index - SLOT * parity, HALF - 1)
    return component(parity, row).astype(F32) * (TWO_PI / length)


def kappa_tile(own, j):
    device = lax.axis_index("gz") * GY + lax.axis_index("gy")
    index_x = jnp.full((GZ, LANES), device * OWN + own, jnp.int32)
    index_y = lax.broadcasted_iota(jnp.int32, (GZ, LANES), 1) + j * LANES
    wave_x = wavenumber(index_x, NX)
    wave_y = wavenumber(index_y, NY)
    return jnp.sqrt(1.0 / (SCREEN * SCREEN) + wave_x * wave_x + wave_y * wave_y)


def message_row(half, g, own, j):
    return pl.ds((half * 8 * GY + g) * BELONG + own * TILES + j, 8, stride=GY * BELONG)


def middle(in_ref, table_ref, out_ref, work_ref, phi_ref):
    lane = lax.broadcasted_iota(jnp.int32, (8, LANES), 1)
    block = OWN * GZ
    for tile in range(block // 8):
        own, half = divmod(tile, GZ // 8)
        arrays = [[in_ref[message_row(half, g, own, j), :] for j in range(TILES)] for g in range(GY)]
        for z, parts in enumerate(swap_chunks(butterfly(arrays), lane)):
            for j in range(TILES):
                work_ref[pl.ds(z * block + tile * 8, 8), lane_tile(j)] = parts[j]
    both_parities(work_ref, table_ref, ((1,), (1,)), phi_ref)

    gz = lax.broadcasted_iota(jnp.int32, (GZ, LANES), 0)
    for own in range(OWN):
        for j in range(TILES):
            kappa = kappa_tile(own, j)
            decay = jnp.exp(-kappa)
            scale = 0.5 / kappa
            hat = [phi_ref[pl.ds(z * block + own * GZ, GZ), lane_tile(j)] for z in range(PLANES)]
            up = [hat[0]]
            for z in range(1, PLANES):
                up.append(decay * up[-1] + hat[z])
            down = [jnp.zeros((GZ, LANES), F32)]
            for z in range(PLANES - 1, 0, -1):
                down.append(decay * (down[-1] + hat[z]))
            down = down[::-1]
            over = up[-1]
            under = decay * (down[0] + hat[0])
            power = decay * decay
            power = power * power
            power = power * power
            step = 1
            while step < GZ:
                over = over + jnp.where(gz >= step, power * pltpu.roll(over, step, 0), 0.0)
                under = under + jnp.where(gz < GZ - step, power * pltpu.roll(under, GZ - step, 0), 0.0)
                power = power * power
                step *= 2
            over = jnp.where(gz >= 1, pltpu.roll(over, 1, 0), 0.0)
            under = jnp.where(gz < GZ - 1, pltpu.roll(under, GZ - 1, 0), 0.0)
            for z in range(PLANES):
                over = decay * over
                up[z] = up[z] + over
            for z in range(PLANES - 1, -1, -1):
                down[z] = down[z] + under
                under = decay * under
            for z in range(PLANES):
                phi_ref[pl.ds(z * block + own * GZ, GZ), lane_tile(j)] = (up[z] + down[z]) * scale

    both_parities(phi_ref, table_ref, ((1,), (0,)), work_ref)
    for tile in range(block // 8):
        own, half = divmod(tile, GZ // 8)
        arrays = [
            [work_ref[pl.ds(z * block + tile * 8, 8), lane_tile(j)] for j in range(TILES)] for z in range(PLANES)
        ]
        for g, parts in enumerate(butterfly(swap_chunks(arrays, lane))):
            for j in range(TILES):
                out_ref[message_row(half, g, own, j), :] = parts[j]


def backward_x(in_ref, table_ref, out_ref, field_ref, flat_ref, sems):
    parts = []
    for parity in range(2):
        rows = [pl.ds(parity * SLOT * TILES + j, SLOT, stride=TILES) for j in range(TILES)]
        value = jnp.concatenate([in_ref[row, :] for row in rows], axis=1)
        parts.append(product(split(jnp.transpose(value)), table_of(table_ref, parity), ((1,), (0,))))
    for side, value in enumerate((parts[0] + parts[1], parts[0] - parts[1])):
        for j in range(2):
            field_ref[2 * side + j] = value[:, lane_tile(j)]
    stores = []
    carry = None
    for piece in range(2 * ROWS):
        y, side = divmod(piece, 2)
        offset = piece * HALF
        shift = offset % LANES
        end = shift + HALF
        tiles = [field_ref[2 * side + j, pl.ds(y, PLANES, stride=CHUNK), :] for j in range(2)]
        if end > PAIR:
            tiles.append(jnp.zeros((PLANES, LANES), F32))
        if shift:
            value = pltpu.roll(jnp.concatenate(tiles, axis=1), shift, 1)
            tiles = [value[:, lane_tile(j)] for j in range(len(tiles))]
        if carry is not None:
            tiles[0] = tiles[0] + carry
        full = end // LANES
        carry = tiles[full] if end % LANES else None
        for j in range(full):
            flat_ref[:, pl.ds(offset - shift + j * LANES, LANES)] = tiles[j]
        if (offset + HALF) % GROUP == 0:
            n = offset // GROUP
            part = pl.ds(n * GROUP, GROUP)
            stores.append(pltpu.make_async_copy(flat_ref.at[:, part], out_ref.at[:, part], sems.at[n]))
            stores[-1].start()
    for store in stores:
        store.wait()


def exchange(buffer):
    whole = buffer.reshape(PEERS, 1, BELONG * LANES)
    whole = lax.all_to_all(whole, ("gz", "gy"), 0, 0, tiled=True)
    return whole.reshape(SEND, LANES)


def on_device(density):
    table_x = jnp.asarray(x_table())
    table_y = jnp.asarray(y_table())
    vmem = pl.BlockSpec(memory_space=pltpu.VMEM)
    hbm = pl.BlockSpec(memory_space=pl.ANY)
    field = pltpu.VMEM((4, PAD, LANES), F32)
    flat = pltpu.VMEM(density.shape, F32)
    square = pltpu.VMEM((PAD, PAD), F32)
    message = pltpu.VMEM((SEND, LANES), F32)
    groups = pltpu.SemaphoreType.DMA((NX * ROWS // GROUP,))

    def here(value):
        return pltpu.with_memory_space_constraint(value, pltpu.VMEM)

    sent = pl.pallas_call(
        forward_x,
        out_shape=message,
        in_specs=[hbm, hbm],
        out_specs=vmem,
        scratch_shapes=[
            field,
            flat,
            pltpu.VMEM(table_x.shape, BF16),
            groups,
            pltpu.SemaphoreType.DMA,
        ],
    )(density, table_x)
    back = pl.pallas_call(
        middle,
        out_shape=message,
        in_specs=[vmem, vmem],
        out_specs=vmem,
        scratch_shapes=[square, square],
    )(here(exchange(sent)), here(table_y))
    return pl.pallas_call(
        backward_x,
        out_shape=jax.ShapeDtypeStruct(density.shape, F32),
        in_specs=[vmem, vmem],
        out_specs=hbm,
        scratch_shapes=[field, flat, groups],
    )(here(exchange(back)), here(table_x))


def solution(mesh):
    return jax.shard_map(
        on_device,
        mesh=mesh,
        in_specs=(P("gz", "gy"),),
        out_specs=P("gz", "gy"),
        check_vma=False,
    )
```

```python
import math

import jax
import jax.numpy as jnp
import numpy as np
from jax import lax
from jax.experimental import pallas as pl
from jax.experimental.pallas import tpu as pltpu
from jax.sharding import PartitionSpec as P

NX = 352
NY = 352
SCREEN = 128
TWO_PI = 2.0 * math.pi

PAD = 384
LANES = 128
TILES = PAD // LANES
HALF = NX // 2
SLOT = PAD // 2
PAIR = 2 * LANES
GZ = 16
GY = 8
PLANES = 8
ROWS = NY // GY
CHUNK = PAD // GY
PITCH = PLANES + 1
PARTS = (0, 24, ROWS)
OWN = 3
PEERS = GZ * GY
SEND = PEERS * OWN * TILES
BELONG = OWN * TILES

F32 = jnp.float32
BF16 = jnp.bfloat16


def component(parity, row):
    return 2 * ((row + 1 - parity) >> 1) + parity


def half_basis(length):
    half = length // 2
    index = np.arange(half)
    basis = np.zeros((2, half, half))
    for parity in range(2):
        for row in range(half):
            m = component(parity, row)
            angle = 2.0 * np.pi * ((m * index) % length) / length
            cosine = row == 0 or (row + parity) % 2 == 1 or m == half
            if parity == 1:
                cosine = row % 2 == 0
            weight = 1.0 if m in (0, half) else 2.0
            basis[parity, row] = (np.cos(angle) if cosine else np.sin(angle)) * np.sqrt(weight / length)
    return basis


def halves(table):
    single = table.astype(np.float32)
    high = single.astype(jnp.bfloat16)
    low = (single - high.astype(np.float32)).astype(jnp.bfloat16)
    return np.stack([high, low])


def x_table():
    table = np.zeros((2, SLOT, PAIR))
    table[:, :HALF, :HALF] = half_basis(NX)
    return halves(table)


def y_table():
    block = np.zeros((2, SLOT, GY // 2, CHUNK))
    block[:, :HALF, :, :ROWS] = half_basis(NY).reshape(2, HALF, GY // 2, ROWS)
    block = block.reshape(2, SLOT, SLOT)
    table = np.zeros((2, PAIR, PAIR))
    table[0, :SLOT, :SLOT] = block[0]
    table[1, PAIR - SLOT :, PAIR - SLOT :] = block[1]
    return halves(table)


def split(value):
    high = value.astype(BF16)
    return high, (value - high.astype(F32)).astype(BF16)


def product(left, right, dims):
    def dot(a, b):
        return lax.dot_general(a, b, (dims, ((), ())), preferred_element_type=F32)

    return dot(left[0], right[0]) + (dot(left[0], right[1]) + dot(left[1], right[0]))


def lane_tile(j):
    return slice(j * LANES, (j + 1) * LANES)


def table_of(table_ref, parity):
    return table_ref[0, parity], table_ref[1, parity]


def shift_lanes(tiles, amount, lane):
    count = len(tiles)
    whole, part = divmod(amount % (count * LANES), LANES)
    if part:
        turned = [pltpu.roll(t, part, 1) for t in tiles]
        tiles = [jnp.where(lane < part, turned[j - 1], turned[j]) for j in range(count)]
    return [tiles[(j - whole) % count] for j in range(count)]


def half_row(ref, offset, lane):
    shift = offset % LANES
    count = -(-(shift + HALF) // LANES)
    tiles = [ref[:, pl.ds(offset - shift + j * LANES, LANES)] for j in range(count)]
    return shift_lanes(tiles, -shift, lane)[:2]


def forward_x(x_ref, table_ref, out_ref, field_ref, flat_ref, local_ref, x_sems, table_sem):
    lane = lax.broadcasted_iota(jnp.int32, (PLANES, LANES), 1)
    loads = []
    for n, (first, last) in enumerate(zip(PARTS, PARTS[1:])):
        part = pl.ds(first * NX, (last - first) * NX)
        loads.append(pltpu.make_async_copy(x_ref.at[:, part], flat_ref.at[:, part], x_sems.at[n]))
    table_load = pltpu.make_async_copy(table_ref, local_ref, table_sem)
    for load in loads:
        load.start()
    table_load.start()
    for y in range(ROWS, CHUNK):
        for j in range(4):
            field_ref[j, pl.ds(y * PITCH, PLANES), :] = jnp.zeros((PLANES, LANES), F32)
    for load, first, last in zip(loads, PARTS, PARTS[1:]):
        load.wait()
        for y in range(first, last):
            one = half_row(flat_ref, y * NX, lane)
            two = half_row(flat_ref, y * NX + HALF, lane)
            for j in range(2):
                field_ref[j, pl.ds(y * PITCH, PLANES), :] = one[j] + two[j]
                field_ref[2 + j, pl.ds(y * PITCH, PLANES), :] = one[j] - two[j]
    table_load.wait()
    for parity in range(2):
        columns = []
        for j in range(2):
            rows = [
                field_ref[2 * parity + j, pl.ds(z + y * PITCH, 8, stride=PITCH), :]
                for z in range(PLANES)
                for y in range(0, CHUNK, 8)
            ]
            columns.append(jnp.concatenate(rows, axis=0))
        field = jnp.concatenate(columns, axis=1)
        result = product(table_of(local_ref, parity), split(field), ((1,), (1,)))
        for j in range(TILES):
            out_ref[pl.ds(parity * SLOT * TILES + j, SLOT, stride=TILES), :] = result[:, lane_tile(j)]


def chunk_pick(parts, lane):
    out = []
    for j in range(TILES):
        first = j * LANES // CHUNK
        last = ((j + 1) * LANES - 1) // CHUNK
        value = parts[last][j]
        for c in range(last - 1, first - 1, -1):
            value = jnp.where(lane < (c + 1) * CHUNK - j * LANES, parts[c][j], value)
        out.append(value)
    return out


def swap_chunks(arrays, lane):
    turned = []
    for d in range(GY):
        picked = chunk_pick([arrays[(c + d) % GY] for c in range(GY)], lane)
        turned.append(shift_lanes(picked, CHUNK * d, lane))
    return [chunk_pick([turned[(c - b) % GY] for c in range(GY)], lane) for b in range(GY)]


def butterfly(arrays):
    pairs = [list(zip(arrays[g], arrays[g + GY // 2])) for g in range(GY // 2)]
    return [[a + b for a, b in p] for p in pairs] + [[a - b for a, b in p] for p in pairs]


def both_parities(value_ref, table_ref, dims, out_ref):
    even = product(split(value_ref[:, :PAIR]), table_of(table_ref, 0), dims)
    odd = product(split(value_ref[:, PAD - PAIR :]), table_of(table_ref, 1), dims)
    out_ref[:, lane_tile(0)] = even[:, :LANES]
    out_ref[:, lane_tile(1)] = even[:, LANES:] + odd[:, :LANES]
    out_ref[:, lane_tile(2)] = odd[:, LANES:]


def wavenumber(index, length):
    parity = (index >= SLOT).astype(jnp.int32)
    row = jnp.minimum(index - SLOT * parity, HALF - 1)
    return component(parity, row).astype(F32) * (TWO_PI / length)


def kappa_tile(own, j):
    device = lax.axis_index("gz") * GY + lax.axis_index("gy")
    index_x = jnp.full((GZ, LANES), device * OWN + own, jnp.int32)
    index_y = lax.broadcasted_iota(jnp.int32, (GZ, LANES), 1) + j * LANES
    wave_x = wavenumber(index_x, NX)
    wave_y = wavenumber(index_y, NY)
    return jnp.sqrt(1.0 / (SCREEN * SCREEN) + wave_x * wave_x + wave_y * wave_y)


def message_row(half, g, own, j):
    return pl.ds((half * 8 * GY + g) * BELONG + own * TILES + j, 8, stride=GY * BELONG)


def middle(in_ref, table_ref, out_ref, work_ref, phi_ref):
    lane = lax.broadcasted_iota(jnp.int32, (8, LANES), 1)
    block = OWN * GZ
    for tile in range(block // 8):
        own, half = divmod(tile, GZ // 8)
        arrays = [[in_ref[message_row(half, g, own, j), :] for j in range(TILES)] for g in range(GY)]
        for z, parts in enumerate(swap_chunks(butterfly(arrays), lane)):
            for j in range(TILES):
                work_ref[pl.ds(z * block + tile * 8, 8), lane_tile(j)] = parts[j]
    both_parities(work_ref, table_ref, ((1,), (1,)), phi_ref)

    gz = lax.broadcasted_iota(jnp.int32, (GZ, LANES), 0)
    for own in range(OWN):
        for j in range(TILES):
            kappa = kappa_tile(own, j)
            decay = jnp.exp(-kappa)
            scale = 0.5 / kappa
            hat = [phi_ref[pl.ds(z * block + own * GZ, GZ), lane_tile(j)] for z in range(PLANES)]
            up = [hat[0]]
            for z in range(1, PLANES):
                up.append(decay * up[-1] + hat[z])
            down = [jnp.zeros((GZ, LANES), F32)]
            for z in range(PLANES - 1, 0, -1):
                down.append(decay * (down[-1] + hat[z]))
            down = down[::-1]
            over = up[-1]
            under = decay * (down[0] + hat[0])
            power = decay * decay
            power = power * power
            power = power * power
            step = 1
            while step < GZ:
                over = over + jnp.where(gz >= step, power * pltpu.roll(over, step, 0), 0.0)
                under = under + jnp.where(gz < GZ - step, power * pltpu.roll(under, GZ - step, 0), 0.0)
                power = power * power
                step *= 2
            over = jnp.where(gz >= 1, pltpu.roll(over, 1, 0), 0.0)
            under = jnp.where(gz < GZ - 1, pltpu.roll(under, GZ - 1, 0), 0.0)
            for z in range(PLANES):
                over = decay * over
                up[z] = up[z] + over
            for z in range(PLANES - 1, -1, -1):
                down[z] = down[z] + under
                under = decay * under
            for z in range(PLANES):
                phi_ref[pl.ds(z * block + own * GZ, GZ), lane_tile(j)] = (up[z] + down[z]) * scale

    both_parities(phi_ref, table_ref, ((1,), (0,)), work_ref)
    for tile in range(block // 8):
        own, half = divmod(tile, GZ // 8)
        arrays = [
            [work_ref[pl.ds(z * block + tile * 8, 8), lane_tile(j)] for j in range(TILES)] for z in range(PLANES)
        ]
        for g, parts in enumerate(butterfly(swap_chunks(arrays, lane))):
            for j in range(TILES):
                out_ref[message_row(half, g, own, j), :] = parts[j]


def backward_x(in_ref, table_ref, out_ref, field_ref, flat_ref, sems):
    parts = []
    for parity in range(2):
        rows = [pl.ds(parity * SLOT * TILES + j, SLOT, stride=TILES) for j in range(TILES)]
        value = jnp.concatenate([in_ref[row, :] for row in rows], axis=1)
        parts.append(product(split(jnp.transpose(value)), table_of(table_ref, parity), ((1,), (0,))))
    for side, value in enumerate((parts[0] + parts[1], parts[0] - parts[1])):
        for j in range(2):
            for z in range(PLANES):
                for y in range(0, CHUNK, 8):
                    rows = pl.ds(z + y * PITCH, 8, stride=PITCH)
                    field_ref[2 * side + j, rows, :] = value[z * CHUNK + y : z * CHUNK + y + 8, lane_tile(j)]
    lane = lax.broadcasted_iota(jnp.int32, (PLANES, LANES), 1)
    stores = []
    carry = None
    for piece in range(2 * ROWS):
        y, side = divmod(piece, 2)
        offset = piece * HALF
        shift = offset % LANES
        end = shift + HALF
        tiles = [field_ref[2 * side + j, pl.ds(y * PITCH, PLANES), :] for j in range(2)]
        if end > PAIR:
            tiles.append(jnp.zeros((PLANES, LANES), F32))
        tiles = shift_lanes(tiles, shift, lane)
        if carry is not None:
            tiles[0] = tiles[0] + carry
        full = end // LANES
        carry = tiles[full] if end % LANES else None
        for j in range(full):
            flat_ref[:, pl.ds(offset - shift + j * LANES, LANES)] = tiles[j]
        if side == 1 and y + 1 in PARTS:
            n = PARTS.index(y + 1) - 1
            part = pl.ds(PARTS[n] * NX, (y + 1 - PARTS[n]) * NX)
            stores.append(pltpu.make_async_copy(flat_ref.at[:, part], out_ref.at[:, part], sems.at[n]))
            stores[-1].start()
    for store in stores:
        store.wait()


def exchange(buffer):
    whole = buffer.reshape(PEERS, 1, BELONG * LANES)
    whole = lax.all_to_all(whole, ("gz", "gy"), 0, 0, tiled=True)
    return whole.reshape(SEND, LANES)


def on_device(density):
    table_x = jnp.asarray(x_table())
    table_y = jnp.asarray(y_table())
    vmem = pl.BlockSpec(memory_space=pltpu.VMEM)
    hbm = pl.BlockSpec(memory_space=pl.ANY)
    field = pltpu.VMEM((4, CHUNK * PITCH, LANES), F32)
    flat = pltpu.VMEM(density.shape, F32)
    square = pltpu.VMEM((PAD, PAD), F32)
    message = pltpu.VMEM((SEND, LANES), F32)
    groups = pltpu.SemaphoreType.DMA((len(PARTS) - 1,))

    def here(value):
        return pltpu.with_memory_space_constraint(value, pltpu.VMEM)

    sent = pl.pallas_call(
        forward_x,
        out_shape=message,
        in_specs=[hbm, hbm],
        out_specs=vmem,
        scratch_shapes=[
            field,
            flat,
            pltpu.VMEM(table_x.shape, BF16),
            groups,
            pltpu.SemaphoreType.DMA,
        ],
    )(density, table_x)
    back = pl.pallas_call(
        middle,
        out_shape=message,
        in_specs=[vmem, vmem],
        out_specs=vmem,
        scratch_shapes=[square, square],
    )(here(exchange(sent)), here(table_y))
    return pl.pallas_call(
        backward_x,
        out_shape=jax.ShapeDtypeStruct(density.shape, F32),
        in_specs=[vmem, vmem],
        out_specs=hbm,
        scratch_shapes=[field, flat, groups],
    )(here(exchange(back)), here(table_x))


def solution(mesh):
    return jax.shard_map(
        on_device,
        mesh=mesh,
        in_specs=(P("gz", "gy"),),
        out_specs=P("gz", "gy"),
        check_vma=False,
    )
```

```python
import math

import jax
import jax.numpy as jnp
import numpy as np
from jax import lax
from jax.experimental import pallas as pl
from jax.experimental.pallas import tpu as pltpu
from jax.sharding import Mesh
from jax.sharding import PartitionSpec as P

NX = 352
NY = 352
SCREEN = 128
TWO_PI = 2.0 * math.pi

PAD = 384
LANES = 128
TILES = PAD // LANES
HALF = NX // 2
SLOT = PAD // 2
PAIR = 2 * LANES
GZ = 16
GX = 4
CORES = 2
GY = GX * CORES
PLANES = 8
ROWS = NY // GY
CHUNK = PAD // GY
PITCH = PLANES + 1
PARTS = (0, 24, ROWS)
OWN = 3
CHIPS = GZ * GX
SWAP = SLOT * TILES
STRIDE = CORES * TILES
SEND = SLOT * STRIDE

F32 = jnp.float32
BF16 = jnp.bfloat16


def component(parity, row):
    return 2 * ((row + 1 - parity) >> 1) + parity


def half_basis(length):
    half = length // 2
    index = np.arange(half)
    basis = np.zeros((2, half, half))
    for parity in range(2):
        for row in range(half):
            m = component(parity, row)
            angle = 2.0 * np.pi * ((m * index) % length) / length
            cosine = row == 0 or (row + parity) % 2 == 1 or m == half
            if parity == 1:
                cosine = row % 2 == 0
            weight = 1.0 if m in (0, half) else 2.0
            basis[parity, row] = (np.cos(angle) if cosine else np.sin(angle)) * np.sqrt(weight / length)
    return basis


def halves(table):
    single = table.astype(np.float32)
    high = single.astype(jnp.bfloat16)
    low = (single - high.astype(np.float32)).astype(jnp.bfloat16)
    return np.stack([high, low])


def x_table():
    table = np.zeros((2, SLOT, PAIR))
    table[:, :HALF, :HALF] = half_basis(NX)
    return halves(table)


def y_table():
    block = np.zeros((2, SLOT, GY // 2, CHUNK))
    block[:, :HALF, :, :ROWS] = half_basis(NY).reshape(2, HALF, GY // 2, ROWS)
    block = block.reshape(2, SLOT, SLOT)
    table = np.zeros((2, PAIR, PAIR))
    table[0, :SLOT, :SLOT] = block[0]
    table[1, PAIR - SLOT :, PAIR - SLOT :] = block[1]
    return halves(table)


def split(value):
    high = value.astype(BF16)
    return high, (value - high.astype(F32)).astype(BF16)


def product(left, right, dims):
    def dot(a, b):
        return lax.dot_general(a, b, (dims, ((), ())), preferred_element_type=F32)

    return dot(left[0], right[0]) + (dot(left[0], right[1]) + dot(left[1], right[0]))


def lane_tile(j):
    return slice(j * LANES, (j + 1) * LANES)


def table_of(table_ref, parity):
    return table_ref[0, parity], table_ref[1, parity]


def shift_lanes(tiles, amount, lane):
    count = len(tiles)
    whole, part = divmod(amount % (count * LANES), LANES)
    if part:
        turned = [pltpu.roll(t, part, 1) for t in tiles]
        tiles = [jnp.where(lane < part, turned[j - 1], turned[j]) for j in range(count)]
    return [tiles[(j - whole) % count] for j in range(count)]


def half_row(ref, offset, lane):
    shift = offset % LANES
    count = -(-(shift + HALF) // LANES)
    tiles = [ref[:, pl.ds(offset - shift + j * LANES, LANES)] for j in range(count)]
    return shift_lanes(tiles, -shift, lane)[:2]


def sign_of(parity):
    return (1 - 2 * parity).astype(F32)


def part_of_field(field_ref, parity):
    columns = []
    for j in range(2):
        rows = []
        for z in range(PLANES):
            for y in range(0, CHUNK, 8):
                at = pl.ds(z + y * PITCH, 8, stride=PITCH)
                rows.append(field_ref[j, at, :] + sign_of(parity) * field_ref[2 + j, at, :])
        columns.append(jnp.concatenate(rows, axis=0))
    return jnp.concatenate(columns, axis=1)


def components(field_ref, table_ref, parity, out_ref):
    result = product(table_of(table_ref, parity), split(part_of_field(field_ref, parity)), ((1,), (1,)))
    for j in range(TILES):
        out_ref[pl.ds(j, SLOT, stride=TILES), :] = result[:, lane_tile(j)]


def forward_other(x_ref, table_ref, out_ref, field_ref, local_ref, flat_ref, x_sems, table_sem):
    lane = lax.broadcasted_iota(jnp.int32, (PLANES, LANES), 1)
    loads = []
    for n, (first, last) in enumerate(zip(PARTS, PARTS[1:])):
        part = pl.ds(first * NX, (last - first) * NX)
        loads.append(pltpu.make_async_copy(x_ref.at[:, part], flat_ref.at[:, part], x_sems.at[n]))
    table_load = pltpu.make_async_copy(table_ref, local_ref, table_sem)
    for load in loads:
        load.start()
    table_load.start()
    for y in range(ROWS, CHUNK):
        for j in range(4):
            field_ref[j, pl.ds(y * PITCH, PLANES), :] = jnp.zeros((PLANES, LANES), F32)
    for load, first, last in zip(loads, PARTS, PARTS[1:]):
        load.wait()
        for y in range(first, last):
            for side in range(2):
                tiles = half_row(flat_ref, y * NX + side * HALF, lane)
                for j in range(2):
                    field_ref[2 * side + j, pl.ds(y * PITCH, PLANES), :] = tiles[j]
    table_load.wait()
    components(field_ref, local_ref, 1 - lax.axis_index("core"), out_ref)


def forward_own(field_ref, table_ref, out_ref):
    components(field_ref, table_ref, lax.axis_index("core"), out_ref)


def merge(own_ref, other_ref, out_ref):
    core = lax.axis_index("core")
    for part_ref, at in ((own_ref, core), (other_ref, 1 - core)):
        for j in range(TILES):
            out_ref[pl.ds(at * TILES + j, SLOT, stride=STRIDE), :] = part_ref[pl.ds(j, SLOT, stride=TILES), :]


def pick_other(in_ref, out_ref):
    at = 1 - lax.axis_index("core")
    for j in range(TILES):
        out_ref[pl.ds(j, SLOT, stride=TILES), :] = in_ref[pl.ds(at * TILES + j, SLOT, stride=STRIDE), :]


def chunk_pick(parts, lane):
    out = []
    for j in range(TILES):
        first = j * LANES // CHUNK
        last = ((j + 1) * LANES - 1) // CHUNK
        value = parts[last][j]
        for c in range(last - 1, first - 1, -1):
            value = jnp.where(lane < (c + 1) * CHUNK - j * LANES, parts[c][j], value)
        out.append(value)
    return out


def swap_chunks(arrays, lane):
    turned = []
    for d in range(GY):
        picked = chunk_pick([arrays[(c + d) % GY] for c in range(GY)], lane)
        turned.append(shift_lanes(picked, CHUNK * d, lane))
    return [chunk_pick([turned[(c - b) % GY] for c in range(GY)], lane) for b in range(GY)]


def butterfly(arrays):
    pairs = [list(zip(arrays[g], arrays[g + GY // 2])) for g in range(GY // 2)]
    return [[a + b for a, b in p] for p in pairs] + [[a - b for a, b in p] for p in pairs]


def both_parities(value_ref, table_ref, dims, out_ref):
    even = product(split(value_ref[:, :PAIR]), table_of(table_ref, 0), dims)
    odd = product(split(value_ref[:, PAD - PAIR :]), table_of(table_ref, 1), dims)
    out_ref[:, lane_tile(0)] = even[:, :LANES]
    out_ref[:, lane_tile(1)] = even[:, LANES:] + odd[:, :LANES]
    out_ref[:, lane_tile(2)] = odd[:, LANES:]


def wavenumber(index, length):
    parity = (index >= SLOT).astype(jnp.int32)
    row = jnp.minimum(index - SLOT * parity, HALF - 1)
    return component(parity, row).astype(F32) * (TWO_PI / length)


def kappa_tile(own, j):
    chip = lax.axis_index("gz") * GX + lax.axis_index("x")
    index_x = jnp.full((GZ, LANES), lax.axis_index("core") * SLOT + chip * OWN + own, jnp.int32)
    index_y = lax.broadcasted_iota(jnp.int32, (GZ, LANES), 1) + j * LANES
    wave_x = wavenumber(index_x, NX)
    wave_y = wavenumber(index_y, NY)
    return jnp.sqrt(1.0 / (SCREEN * SCREEN) + wave_x * wave_x + wave_y * wave_y)


def message_row(half, g, own, j):
    x, core = divmod(g, CORES)
    first = ((half * 8 * GX + x) * OWN + own) * STRIDE + core * TILES + j
    return pl.ds(first, 8, stride=GX * OWN * STRIDE)


def middle(in_ref, table_ref, out_ref, work_ref, phi_ref):
    lane = lax.broadcasted_iota(jnp.int32, (8, LANES), 1)
    block = OWN * GZ
    for tile in range(block // 8):
        own, half = divmod(tile, GZ // 8)
        arrays = [[in_ref[message_row(half, g, own, j), :] for j in range(TILES)] for g in range(GY)]
        for z, parts in enumerate(swap_chunks(butterfly(arrays), lane)):
            for j in range(TILES):
                work_ref[pl.ds(z * block + tile * 8, 8), lane_tile(j)] = parts[j]
    both_parities(work_ref, table_ref, ((1,), (1,)), phi_ref)

    gz = lax.broadcasted_iota(jnp.int32, (GZ, LANES), 0)
    for own in range(OWN):
        for j in range(TILES):
            kappa = kappa_tile(own, j)
            decay = jnp.exp(-kappa)
            scale = 0.5 / kappa
            hat = [phi_ref[pl.ds(z * block + own * GZ, GZ), lane_tile(j)] for z in range(PLANES)]
            up = [hat[0]]
            for z in range(1, PLANES):
                up.append(decay * up[-1] + hat[z])
            down = [jnp.zeros((GZ, LANES), F32)]
            for z in range(PLANES - 1, 0, -1):
                down.append(decay * (down[-1] + hat[z]))
            down = down[::-1]
            over = up[-1]
            under = decay * (down[0] + hat[0])
            power = decay * decay
            power = power * power
            power = power * power
            step = 1
            while step < GZ:
                over = over + jnp.where(gz >= step, power * pltpu.roll(over, step, 0), 0.0)
                under = under + jnp.where(gz < GZ - step, power * pltpu.roll(under, GZ - step, 0), 0.0)
                power = power * power
                step *= 2
            over = jnp.where(gz >= 1, pltpu.roll(over, 1, 0), 0.0)
            under = jnp.where(gz < GZ - 1, pltpu.roll(under, GZ - 1, 0), 0.0)
            for z in range(PLANES):
                over = decay * over
                up[z] = up[z] + over
            for z in range(PLANES - 1, -1, -1):
                down[z] = down[z] + under
                under = decay * under
            for z in range(PLANES):
                phi_ref[pl.ds(z * block + own * GZ, GZ), lane_tile(j)] = (up[z] + down[z]) * scale

    both_parities(phi_ref, table_ref, ((1,), (0,)), work_ref)
    for tile in range(block // 8):
        own, half = divmod(tile, GZ // 8)
        arrays = [
            [work_ref[pl.ds(z * block + tile * 8, 8), lane_tile(j)] for j in range(TILES)] for z in range(PLANES)
        ]
        for g, parts in enumerate(butterfly(swap_chunks(arrays, lane))):
            for j in range(TILES):
                out_ref[message_row(half, g, own, j), :] = parts[j]


def contribution(value, table_ref, parity):
    return product(split(jnp.transpose(value)), table_of(table_ref, parity), ((1,), (0,)))


def backward_own(in_ref, table_ref, out_ref):
    core = lax.axis_index("core")
    rows = [pl.ds(core * TILES + j, SLOT, stride=STRIDE) for j in range(TILES)]
    value = jnp.concatenate([in_ref[row, :] for row in rows], axis=1)
    out_ref[...] = contribution(value, table_ref, core)


def backward_other(in_ref, own_ref, table_ref, out_ref, field_ref, flat_ref, sems):
    core = lax.axis_index("core")
    rows = [pl.ds(j, SLOT, stride=TILES) for j in range(TILES)]
    value = jnp.concatenate([in_ref[row, :] for row in rows], axis=1)
    other = contribution(value, table_ref, 1 - core)
    own = own_ref[...]
    for side, value in enumerate((own + other, (own - other) * sign_of(core))):
        for j in range(2):
            for z in range(PLANES):
                for y in range(0, CHUNK, 8):
                    rows = pl.ds(z + y * PITCH, 8, stride=PITCH)
                    field_ref[2 * side + j, rows, :] = value[z * CHUNK + y : z * CHUNK + y + 8, lane_tile(j)]
    lane = lax.broadcasted_iota(jnp.int32, (PLANES, LANES), 1)
    stores = []
    carry = None
    for piece in range(2 * ROWS):
        y, side = divmod(piece, 2)
        offset = piece * HALF
        shift = offset % LANES
        end = shift + HALF
        tiles = [field_ref[2 * side + j, pl.ds(y * PITCH, PLANES), :] for j in range(2)]
        if end > PAIR:
            tiles.append(jnp.zeros((PLANES, LANES), F32))
        tiles = shift_lanes(tiles, shift, lane)
        if carry is not None:
            tiles[0] = tiles[0] + carry
        full = end // LANES
        carry = tiles[full] if end % LANES else None
        for j in range(full):
            flat_ref[:, pl.ds(offset - shift + j * LANES, LANES)] = tiles[j]
        if side == 1 and y + 1 in PARTS:
            n = PARTS.index(y + 1) - 1
            part = pl.ds(PARTS[n] * NX, (y + 1 - PARTS[n]) * NX)
            stores.append(pltpu.make_async_copy(flat_ref.at[:, part], out_ref.at[:, part], sems.at[n]))
            stores[-1].start()
    for store in stores:
        store.wait()


def exchange(buffer):
    whole = buffer.reshape(CHIPS, 1, SEND // CHIPS * LANES)
    whole = lax.all_to_all(whole, ("gz", "x"), 0, 0, tiled=True)
    return whole.reshape(SEND, LANES)


def swap_cores(buffer):
    return lax.ppermute(buffer, "core", [(0, 1), (1, 0)])


def on_device(density):
    table_x = jnp.asarray(x_table())
    table_y = jnp.asarray(y_table())
    vmem = pl.BlockSpec(memory_space=pltpu.VMEM)
    hbm = pl.BlockSpec(memory_space=pl.ANY)
    field = pltpu.VMEM((4, CHUNK * PITCH, LANES), F32)
    flat = pltpu.VMEM(density.shape, F32)
    square = pltpu.VMEM((PAD, PAD), F32)
    message = pltpu.VMEM((SEND, LANES), F32)
    half = pltpu.VMEM((SWAP, LANES), F32)
    copies = pltpu.SemaphoreType.DMA((len(PARTS) - 1,))

    def here(value):
        return pltpu.with_memory_space_constraint(value, pltpu.VMEM)

    def call(kernel, out_shape, *args):
        return pl.pallas_call(
            kernel, out_shape=out_shape, in_specs=[vmem] * len(args), out_specs=vmem
        )(*(here(a) for a in args))

    give, fields, local_x = pl.pallas_call(
        forward_other,
        out_shape=(half, field, pltpu.VMEM(table_x.shape, BF16)),
        in_specs=[hbm, hbm],
        out_specs=(vmem, vmem, vmem),
        scratch_shapes=[flat, copies, pltpu.SemaphoreType.DMA],
    )(density, table_x)
    taken = swap_cores(give)
    kept = call(forward_own, half, fields, local_x)
    held = exchange(call(merge, message, kept, taken))

    back = pl.pallas_call(
        middle,
        out_shape=message,
        in_specs=[vmem, vmem],
        out_specs=vmem,
        scratch_shapes=[square, square],
    )(here(held), here(table_y))

    held = exchange(back)
    taken = swap_cores(call(pick_other, half, held))
    kept = call(backward_own, pltpu.VMEM((PAD, PAIR), F32), held, table_x)
    return pl.pallas_call(
        backward_other,
        out_shape=jax.ShapeDtypeStruct(density.shape, F32),
        in_specs=[vmem, vmem, vmem],
        out_specs=hbm,
        scratch_shapes=[field, flat, copies],
    )(here(taken), here(kept), here(table_x))


def solution(mesh):
    chips = Mesh(mesh.devices.reshape(GZ, GX, CORES), ("gz", "x", "core"))
    spec = P("gz", ("x", "core"))
    return jax.shard_map(
        on_device,
        mesh=chips,
        in_specs=(spec,),
        out_specs=spec,
        check_vma=False,
    )
```

```python
import math

import jax
import jax.numpy as jnp
import numpy as np
from jax import lax
from jax.experimental import pallas as pl
from jax.experimental.pallas import tpu as pltpu
from jax.sharding import Mesh
from jax.sharding import PartitionSpec as P

NX = 352
NY = 352
SCREEN = 128
TWO_PI = 2.0 * math.pi

PAD = 384
LANES = 128
TILES = PAD // LANES
HALF = NX // 2
SLOT = PAD // 2
PAIR = 2 * LANES
GZ = 16
GX = 4
CORES = 2
GY = GX * CORES
PLANES = 8
ROWS = NY // GY
CHUNK = PAD // GY
PITCH = PLANES + 1
BLOCKS = (0, 16, 32, CHUNK)
PARTS = (0, 24, ROWS)
OWN = 3
PEERS = GZ * GY
SEND = PEERS * OWN * TILES
BELONG = OWN * TILES

F32 = jnp.float32
BF16 = jnp.bfloat16


def component(parity, row):
    return 2 * ((row + 1 - parity) >> 1) + parity


def half_basis(length):
    half = length // 2
    index = np.arange(half)
    basis = np.zeros((2, half, half))
    for parity in range(2):
        for row in range(half):
            m = component(parity, row)
            angle = 2.0 * np.pi * ((m * index) % length) / length
            cosine = row == 0 or (row + parity) % 2 == 1 or m == half
            if parity == 1:
                cosine = row % 2 == 0
            weight = 1.0 if m in (0, half) else 2.0
            basis[parity, row] = (np.cos(angle) if cosine else np.sin(angle)) * np.sqrt(weight / length)
    return basis


def halves(table):
    single = table.astype(np.float32)
    high = single.astype(jnp.bfloat16)
    low = (single - high.astype(np.float32)).astype(jnp.bfloat16)
    return np.stack([high, low])


def x_table():
    table = np.zeros((2, SLOT, PAIR))
    table[:, :HALF, :HALF] = half_basis(NX)
    return halves(table)


def y_table():
    block = np.zeros((2, SLOT, GY // 2, CHUNK))
    block[:, :HALF, :, :ROWS] = half_basis(NY).reshape(2, HALF, GY // 2, ROWS)
    block = block.reshape(2, SLOT, SLOT)
    table = np.zeros((2, PAIR, PAIR))
    table[0, :SLOT, :SLOT] = block[0]
    table[1, PAIR - SLOT :, PAIR - SLOT :] = block[1]
    return halves(table)


def split(value):
    high = value.astype(BF16)
    return high, (value - high.astype(F32)).astype(BF16)


def product(left, right, dims):
    def dot(a, b):
        return lax.dot_general(a, b, (dims, ((), ())), preferred_element_type=F32)

    return dot(left[0], right[0]) + (dot(left[0], right[1]) + dot(left[1], right[0]))


def lane_tile(j):
    return slice(j * LANES, (j + 1) * LANES)


def table_of(table_ref, parity):
    return table_ref[0, parity], table_ref[1, parity]


def shift_lanes(tiles, amount, lane):
    count = len(tiles)
    whole, part = divmod(amount % (count * LANES), LANES)
    if part:
        turned = [pltpu.roll(t, part, 1) for t in tiles]
        tiles = [jnp.where(lane < part, turned[j - 1], turned[j]) for j in range(count)]
    return [tiles[(j - whole) % count] for j in range(count)]


def half_row(ref, offset, lane):
    shift = offset % LANES
    count = -(-(shift + HALF) // LANES)
    tiles = [ref[:, pl.ds(offset - shift + j * LANES, LANES)] for j in range(count)]
    return shift_lanes(tiles, -shift, lane)[:2]


def forward_x(x_ref, table_ref, out_ref, field_ref, flat_ref, local_ref, x_sems, table_sem):
    lane = lax.broadcasted_iota(jnp.int32, (PLANES, LANES), 1)
    loads = []
    for n, (first, last) in enumerate(zip(PARTS, PARTS[1:])):
        part = pl.ds(first * NX, (last - first) * NX)
        loads.append(pltpu.make_async_copy(x_ref.at[:, part], flat_ref.at[:, part], x_sems.at[n]))
    table_load = pltpu.make_async_copy(table_ref, local_ref, table_sem)
    for load in loads:
        load.start()
    table_load.start()
    for y in range(ROWS, CHUNK):
        for j in range(4):
            field_ref[j, pl.ds(y * PITCH, PLANES), :] = jnp.zeros((PLANES, LANES), F32)
    for load, first, last in zip(loads, PARTS, PARTS[1:]):
        load.wait()
        for y in range(first, last):
            one = half_row(flat_ref, y * NX, lane)
            two = half_row(flat_ref, y * NX + HALF, lane)
            for j in range(2):
                field_ref[j, pl.ds(y * PITCH, PLANES), :] = one[j] + two[j]
                field_ref[2 + j, pl.ds(y * PITCH, PLANES), :] = one[j] - two[j]
    table_load.wait()
    for parity in range(2):
        columns = []
        for j in range(2):
            rows = [
                field_ref[2 * parity + j, pl.ds(z + y * PITCH, 8, stride=PITCH), :]
                for z in range(PLANES)
                for y in range(0, CHUNK, 8)
            ]
            columns.append(jnp.concatenate(rows, axis=0))
        field = jnp.concatenate(columns, axis=1)
        result = product(table_of(local_ref, parity), split(field), ((1,), (1,)))
        for j in range(TILES):
            out_ref[pl.ds(parity * SLOT * TILES + j, SLOT, stride=TILES), :] = result[:, lane_tile(j)]


def chunk_pick(parts, lane):
    out = []
    for j in range(TILES):
        first = j * LANES // CHUNK
        last = ((j + 1) * LANES - 1) // CHUNK
        value = parts[last][j]
        for c in range(last - 1, first - 1, -1):
            value = jnp.where(lane < (c + 1) * CHUNK - j * LANES, parts[c][j], value)
        out.append(value)
    return out


def swap_chunks(arrays, lane):
    turned = []
    for d in range(GY):
        picked = chunk_pick([arrays[(c + d) % GY] for c in range(GY)], lane)
        turned.append(shift_lanes(picked, CHUNK * d, lane))
    return [chunk_pick([turned[(c - b) % GY] for c in range(GY)], lane) for b in range(GY)]


def butterfly(arrays):
    pairs = [list(zip(arrays[g], arrays[g + GY // 2])) for g in range(GY // 2)]
    return [[a + b for a, b in p] for p in pairs] + [[a - b for a, b in p] for p in pairs]


def both_parities(value_ref, table_ref, dims, out_ref):
    even = product(split(value_ref[:, :PAIR]), table_of(table_ref, 0), dims)
    odd = product(split(value_ref[:, PAD - PAIR :]), table_of(table_ref, 1), dims)
    out_ref[:, lane_tile(0)] = even[:, :LANES]
    out_ref[:, lane_tile(1)] = even[:, LANES:] + odd[:, :LANES]
    out_ref[:, lane_tile(2)] = odd[:, LANES:]


def wavenumber(index, length):
    parity = (index >= SLOT).astype(jnp.int32)
    row = jnp.minimum(index - SLOT * parity, HALF - 1)
    return component(parity, row).astype(F32) * (TWO_PI / length)


def kappa_tile(own, j):
    place = (lax.axis_index("core") * GZ + lax.axis_index("gz")) * GX + lax.axis_index("x")
    index_x = jnp.full((GZ, LANES), place * OWN + own, jnp.int32)
    index_y = lax.broadcasted_iota(jnp.int32, (GZ, LANES), 1) + j * LANES
    wave_x = wavenumber(index_x, NX)
    wave_y = wavenumber(index_y, NY)
    return jnp.sqrt(1.0 / (SCREEN * SCREEN) + wave_x * wave_x + wave_y * wave_y)


def message_row(half, g, own, j):
    x, core = divmod(g, CORES)
    first = ((core * GZ + half * 8) * GX + x) * BELONG + own * TILES + j
    return pl.ds(first, 8, stride=GX * BELONG)


def middle(in_ref, table_ref, out_ref, work_ref, phi_ref):
    lane = lax.broadcasted_iota(jnp.int32, (8, LANES), 1)
    block = OWN * GZ
    for tile in range(block // 8):
        own, half = divmod(tile, GZ // 8)
        arrays = [[in_ref[message_row(half, g, own, j), :] for j in range(TILES)] for g in range(GY)]
        for z, parts in enumerate(swap_chunks(butterfly(arrays), lane)):
            for j in range(TILES):
                work_ref[pl.ds(z * block + tile * 8, 8), lane_tile(j)] = parts[j]
    both_parities(work_ref, table_ref, ((1,), (1,)), phi_ref)

    gz = lax.broadcasted_iota(jnp.int32, (GZ, LANES), 0)
    for own in range(OWN):
        for j in range(TILES):
            kappa = kappa_tile(own, j)
            decay = jnp.exp(-kappa)
            scale = 0.5 / kappa
            hat = [phi_ref[pl.ds(z * block + own * GZ, GZ), lane_tile(j)] for z in range(PLANES)]
            over = hat[0]
            for z in range(1, PLANES):
                over = decay * over + hat[z]
            under = hat[-1]
            for z in range(PLANES - 2, -1, -1):
                under = decay * under + hat[z]
            under = decay * under
            power = decay * decay
            power = power * power
            power = power * power
            step = 1
            while step < GZ:
                over = over + jnp.where(gz >= step, power * pltpu.roll(over, step, 0), 0.0)
                under = under + jnp.where(gz < GZ - step, power * pltpu.roll(under, GZ - step, 0), 0.0)
                power = power * power
                step *= 2
            over = jnp.where(gz >= 1, pltpu.roll(over, 1, 0), 0.0)
            under = jnp.where(gz < GZ - 1, pltpu.roll(under, GZ - 1, 0), 0.0)
            down = []
            for z in range(PLANES - 1, -1, -1):
                down.append(under)
                under = decay * (under + hat[z])
            for z in range(PLANES):
                over = decay * over + hat[z]
                phi_ref[pl.ds(z * block + own * GZ, GZ), lane_tile(j)] = (over + down[PLANES - 1 - z]) * scale

    both_parities(phi_ref, table_ref, ((1,), (0,)), work_ref)
    for tile in range(block // 8):
        own, half = divmod(tile, GZ // 8)
        arrays = [
            [work_ref[pl.ds(z * block + tile * 8, 8), lane_tile(j)] for j in range(TILES)] for z in range(PLANES)
        ]
        for g, parts in enumerate(butterfly(swap_chunks(arrays, lane))):
            for j in range(TILES):
                out_ref[message_row(half, g, own, j), :] = parts[j]


def backward_x(in_ref, table_ref, out_ref, field_ref, flat_ref, sems):
    lane = lax.broadcasted_iota(jnp.int32, (PLANES, LANES), 1)
    turned = []
    for parity in range(2):
        rows = [pl.ds(parity * SLOT * TILES + j, SLOT, stride=TILES) for j in range(TILES)]
        turned.append(jnp.transpose(jnp.concatenate([in_ref[row, :] for row in rows], axis=1)))
    stores = []
    carry = None
    for n, (first, last) in enumerate(zip(BLOCKS, BLOCKS[1:])):
        tops = [z * CHUNK + y for z in range(PLANES) for y in range(first, last, 8)]
        parts = []
        for parity in range(2):
            value = jnp.concatenate([turned[parity][t : t + 8] for t in tops], axis=0)
            parts.append(product(split(value), table_of(table_ref, parity), ((1,), (0,))))
        for side, value in enumerate((parts[0] + parts[1], parts[0] - parts[1])):
            for j in range(2):
                for i, t in enumerate(tops):
                    z, y = divmod(t, CHUNK)
                    rows = pl.ds(z + y * PITCH, 8, stride=PITCH)
                    field_ref[2 * side + j, rows, :] = value[8 * i : 8 * i + 8, lane_tile(j)]
        for piece in range(2 * first, 2 * min(last, ROWS)):
            y, side = divmod(piece, 2)
            offset = piece * HALF
            shift = offset % LANES
            end = shift + HALF
            tiles = [field_ref[2 * side + j, pl.ds(y * PITCH, PLANES), :] for j in range(2)]
            if end > PAIR:
                tiles.append(jnp.zeros((PLANES, LANES), F32))
            tiles = shift_lanes(tiles, shift, lane)
            if carry is not None:
                tiles[0] = tiles[0] + carry
            full = end // LANES
            carry = tiles[full] if end % LANES else None
            for j in range(full):
                flat_ref[:, pl.ds(offset - shift + j * LANES, LANES)] = tiles[j]
        part = pl.ds(first * NX, (min(last, ROWS) - first) * NX)
        stores.append(pltpu.make_async_copy(flat_ref.at[:, part], out_ref.at[:, part], sems.at[n]))
        stores[-1].start()
    for store in stores:
        store.wait()


def exchange(buffer):
    whole = buffer.reshape(PEERS, 1, BELONG * LANES)
    whole = lax.all_to_all(whole, ("core", "gz", "x"), 0, 0, tiled=True)
    return whole.reshape(SEND, LANES)


def on_device(density):
    table_x = jnp.asarray(x_table())
    table_y = jnp.asarray(y_table())
    vmem = pl.BlockSpec(memory_space=pltpu.VMEM)
    hbm = pl.BlockSpec(memory_space=pl.ANY)
    field = pltpu.VMEM((4, CHUNK * PITCH, LANES), F32)
    flat = pltpu.VMEM(density.shape, F32)
    square = pltpu.VMEM((PAD, PAD), F32)
    message = pltpu.VMEM((SEND, LANES), F32)
    groups = pltpu.SemaphoreType.DMA((len(PARTS) - 1,))

    def here(value):
        return pltpu.with_memory_space_constraint(value, pltpu.VMEM)

    sent = pl.pallas_call(
        forward_x,
        out_shape=message,
        in_specs=[hbm, hbm],
        out_specs=vmem,
        scratch_shapes=[
            field,
            flat,
            pltpu.VMEM(table_x.shape, BF16),
            groups,
            pltpu.SemaphoreType.DMA,
        ],
    )(density, table_x)
    back = pl.pallas_call(
        middle,
        out_shape=message,
        in_specs=[vmem, vmem],
        out_specs=vmem,
        scratch_shapes=[square, square],
    )(here(exchange(sent)), here(table_y))
    return pl.pallas_call(
        backward_x,
        out_shape=jax.ShapeDtypeStruct(density.shape, F32),
        in_specs=[vmem, vmem],
        out_specs=hbm,
        scratch_shapes=[field, flat, pltpu.SemaphoreType.DMA((len(BLOCKS) - 1,))],
    )(here(exchange(back)), here(table_x))


def solution(mesh):
    split_rows = Mesh(mesh.devices.reshape(GZ, GX, CORES), ("gz", "x", "core"))
    spec = P("gz", ("x", "core"))
    return jax.shard_map(
        on_device,
        mesh=split_rows,
        in_specs=(spec,),
        out_specs=spec,
        check_vma=False,
    )
```

```python
import math

import jax
import jax.numpy as jnp
import numpy as np
from jax import lax
from jax.experimental import pallas as pl
from jax.experimental.pallas import tpu as pltpu
from jax.sharding import Mesh
from jax.sharding import PartitionSpec as P

NX = 352
NY = 352
SCREEN = 128
TWO_PI = 2.0 * math.pi

PAD = 384
LANES = 128
TILES = PAD // LANES
HALF = NX // 2
SLOT = PAD // 2
PAIR = 2 * LANES
GZ = 16
GX = 4
CORES = 2
GY = GX * CORES
PLANES = 8
ROWS = NY // GY
CHUNK = PAD // GY
PITCH = PLANES + 1
BLOCKS = (0, 16, 32, CHUNK)
PARTS = (0, 24, ROWS)
OWN = 3
PEERS = GZ * GY
SEND = PEERS * OWN * TILES
BELONG = OWN * TILES

F32 = jnp.float32
BF16 = jnp.bfloat16


def component(parity, row):
    return 2 * ((row + 1 - parity) >> 1) + parity


def half_basis(length):
    half = length // 2
    index = np.arange(half)
    basis = np.zeros((2, half, half))
    for parity in range(2):
        for row in range(half):
            m = component(parity, row)
            angle = 2.0 * np.pi * ((m * index) % length) / length
            cosine = row == 0 or (row + parity) % 2 == 1 or m == half
            if parity == 1:
                cosine = row % 2 == 0
            weight = 1.0 if m in (0, half) else 2.0
            basis[parity, row] = (np.cos(angle) if cosine else np.sin(angle)) * np.sqrt(weight / length)
    return basis


def halves(table):
    single = table.astype(np.float32)
    high = single.astype(jnp.bfloat16)
    low = (single - high.astype(np.float32)).astype(jnp.bfloat16)
    return np.stack([high, low])


def x_table():
    table = np.zeros((2, SLOT, PAIR))
    table[:, :HALF, :HALF] = half_basis(NX)
    return halves(table)


def y_table():
    block = np.zeros((2, SLOT, GY // 2, CHUNK))
    block[:, :HALF, :, :ROWS] = half_basis(NY).reshape(2, HALF, GY // 2, ROWS)
    block = block.reshape(2, SLOT, SLOT)
    table = np.zeros((2, PAIR, PAIR))
    table[0, :SLOT, :SLOT] = block[0]
    table[1, PAIR - SLOT :, PAIR - SLOT :] = block[1]
    return halves(table)


def split(value):
    high = value.astype(BF16)
    return high, (value - high.astype(F32)).astype(BF16)


def product(left, right, dims):
    def dot(a, b):
        return lax.dot_general(a, b, (dims, ((), ())), preferred_element_type=F32)

    return dot(left[0], right[0]) + (dot(left[0], right[1]) + dot(left[1], right[0]))


def lane_tile(j):
    return slice(j * LANES, (j + 1) * LANES)


def table_of(table_ref, parity):
    return table_ref[0, parity], table_ref[1, parity]


def shift_lanes(tiles, amount, lane):
    count = len(tiles)
    whole, part = divmod(amount % (count * LANES), LANES)
    if part:
        turned = [pltpu.roll(t, part, 1) for t in tiles]
        tiles = [jnp.where(lane < part, turned[j - 1], turned[j]) for j in range(count)]
    return [tiles[(j - whole) % count] for j in range(count)]


def half_row(ref, offset, lane):
    shift = offset % LANES
    count = -(-(shift + HALF) // LANES)
    tiles = [ref[:, pl.ds(offset - shift + j * LANES, LANES)] for j in range(count)]
    return shift_lanes(tiles, -shift, lane)[:2]


def forward_x(x_ref, table_ref, out_ref, decay_ref, scale_ref, field_ref, flat_ref, local_ref, x_sems, table_sem):
    lane = lax.broadcasted_iota(jnp.int32, (PLANES, LANES), 1)
    loads = []
    for n, (first, last) in enumerate(zip(PARTS, PARTS[1:])):
        part = pl.ds(first * NX, (last - first) * NX)
        loads.append(pltpu.make_async_copy(x_ref.at[:, part], flat_ref.at[:, part], x_sems.at[n]))
    table_load = pltpu.make_async_copy(table_ref, local_ref, table_sem)
    for load in loads:
        load.start()
    table_load.start()
    for own in range(OWN):
        for j in range(TILES):
            kappa = kappa_tile(own, j)
            decay_ref[pl.ds(8 * own, 8), lane_tile(j)] = jnp.exp(-kappa)
            scale_ref[pl.ds(8 * own, 8), lane_tile(j)] = 0.5 / kappa
    for y in range(ROWS, CHUNK):
        for j in range(4):
            field_ref[j, pl.ds(y * PITCH, PLANES), :] = jnp.zeros((PLANES, LANES), F32)
    for load, first, last in zip(loads, PARTS, PARTS[1:]):
        load.wait()
        for y in range(first, last):
            one = half_row(flat_ref, y * NX, lane)
            two = half_row(flat_ref, y * NX + HALF, lane)
            for j in range(2):
                field_ref[j, pl.ds(y * PITCH, PLANES), :] = one[j] + two[j]
                field_ref[2 + j, pl.ds(y * PITCH, PLANES), :] = one[j] - two[j]
    table_load.wait()
    for parity in range(2):
        columns = []
        for j in range(2):
            rows = [
                field_ref[2 * parity + j, pl.ds(z + y * PITCH, 8, stride=PITCH), :]
                for z in range(PLANES)
                for y in range(0, CHUNK, 8)
            ]
            columns.append(jnp.concatenate(rows, axis=0))
        field = jnp.concatenate(columns, axis=1)
        result = product(table_of(local_ref, parity), split(field), ((1,), (1,)))
        for j in range(TILES):
            out_ref[pl.ds(parity * SLOT * TILES + j, SLOT, stride=TILES), :] = result[:, lane_tile(j)]


def chunk_pick(parts, lane):
    out = []
    for j in range(TILES):
        first = j * LANES // CHUNK
        last = ((j + 1) * LANES - 1) // CHUNK
        value = parts[last][j]
        for c in range(last - 1, first - 1, -1):
            value = jnp.where(lane < (c + 1) * CHUNK - j * LANES, parts[c][j], value)
        out.append(value)
    return out


def swap_chunks(arrays, lane):
    turned = []
    for d in range(GY):
        picked = chunk_pick([arrays[(c + d) % GY] for c in range(GY)], lane)
        turned.append(shift_lanes(picked, CHUNK * d, lane))
    return [chunk_pick([turned[(c - b) % GY] for c in range(GY)], lane) for b in range(GY)]


def butterfly(arrays):
    pairs = [list(zip(arrays[g], arrays[g + GY // 2])) for g in range(GY // 2)]
    return [[a + b for a, b in p] for p in pairs] + [[a - b for a, b in p] for p in pairs]


def both_parities(value_ref, table_ref, dims, out_ref, rows):
    even = product(split(value_ref[rows, :PAIR]), table_of(table_ref, 0), dims)
    odd = product(split(value_ref[rows, PAD - PAIR :]), table_of(table_ref, 1), dims)
    out_ref[rows, lane_tile(0)] = even[:, :LANES]
    out_ref[rows, lane_tile(1)] = even[:, LANES:] + odd[:, :LANES]
    out_ref[rows, lane_tile(2)] = odd[:, LANES:]


def wavenumber(index, length):
    parity = (index >= SLOT).astype(jnp.int32)
    row = jnp.minimum(index - SLOT * parity, HALF - 1)
    return component(parity, row).astype(F32) * (TWO_PI / length)


def kappa_tile(own, j):
    place = (lax.axis_index("core") * GZ + lax.axis_index("gz")) * GX + lax.axis_index("x")
    index_x = jnp.full((8, LANES), place * OWN + own, jnp.int32)
    index_y = lax.broadcasted_iota(jnp.int32, (8, LANES), 1) + j * LANES
    wave_x = wavenumber(index_x, NX)
    wave_y = wavenumber(index_y, NY)
    return jnp.sqrt(1.0 / (SCREEN * SCREEN) + wave_x * wave_x + wave_y * wave_y)


def message_row(half, g, own, j):
    x, core = divmod(g, CORES)
    first = ((core * GZ + half * 8) * GX + x) * BELONG + own * TILES + j
    return pl.ds(first, 8, stride=GX * BELONG)


def plane_row(own, z, half=0):
    return own * PLANES * GZ + z * GZ + half * 8


def gather(own, lane, in_ref, work_ref):
    for half in range(GZ // 8):
        arrays = [[in_ref[message_row(half, g, own, j), :] for j in range(TILES)] for g in range(GY)]
        for z, parts in enumerate(swap_chunks(butterfly(arrays), lane)):
            for j in range(TILES):
                work_ref[pl.ds(plane_row(own, z, half), 8), lane_tile(j)] = parts[j]


def scatter(own, lane, work_ref, out_ref):
    for half in range(GZ // 8):
        arrays = [
            [work_ref[pl.ds(plane_row(own, z, half), 8), lane_tile(j)] for j in range(TILES)] for z in range(PLANES)
        ]
        for g, parts in enumerate(butterfly(swap_chunks(arrays, lane))):
            for j in range(TILES):
                out_ref[message_row(half, g, own, j), :] = parts[j]


def decaying_sums(own, gz, decay_ref, scale_ref, phi_ref):
    for j in range(TILES):
        decay = decay_ref[pl.ds(8 * own, 8), lane_tile(j)]
        scale = scale_ref[pl.ds(8 * own, 8), lane_tile(j)]
        power = decay * decay
        power = power * power
        power = power * power
        decay, scale, power = (jnp.concatenate([t] * (GZ // 8), axis=0) for t in (decay, scale, power))
        hat = [phi_ref[pl.ds(plane_row(own, z), GZ), lane_tile(j)] for z in range(PLANES)]
        over = hat[0]
        for z in range(1, PLANES):
            over = decay * over + hat[z]
        under = hat[-1]
        for z in range(PLANES - 2, -1, -1):
            under = decay * under + hat[z]
        under = decay * under
        step = 1
        while step < GZ:
            over = over + jnp.where(gz >= step, power * pltpu.roll(over, step, 0), 0.0)
            under = under + jnp.where(gz < GZ - step, power * pltpu.roll(under, GZ - step, 0), 0.0)
            power = power * power
            step *= 2
        over = jnp.where(gz >= 1, pltpu.roll(over, 1, 0), 0.0)
        under = jnp.where(gz < GZ - 1, pltpu.roll(under, GZ - 1, 0), 0.0)
        down = []
        for z in range(PLANES - 1, -1, -1):
            down.append(under)
            under = decay * (under + hat[z])
        for z in range(PLANES):
            over = decay * over + hat[z]
            phi_ref[pl.ds(plane_row(own, z), GZ), lane_tile(j)] = (over + down[PLANES - 1 - z]) * scale


def middle(in_ref, table_ref, decay_ref, scale_ref, out_ref, work_ref, phi_ref, back_ref):
    lane = lax.broadcasted_iota(jnp.int32, (8, LANES), 1)
    gz = lax.broadcasted_iota(jnp.int32, (GZ, LANES), 0)
    forth = ((1,), (1,))
    back = ((1,), (0,))
    every = pl.ds(0, PAD)

    def rows(own):
        return pl.ds(own * PLANES * GZ, PLANES * GZ)

    first = pl.ds(0, PLANES * GZ)
    rest = pl.ds(PLANES * GZ, (OWN - 1) * PLANES * GZ)
    for own in range(OWN):
        gather(own, lane, in_ref, work_ref)
    both_parities(work_ref, table_ref, forth, phi_ref, first)
    both_parities(work_ref, table_ref, forth, phi_ref, rest)
    decaying_sums(0, gz, decay_ref, scale_ref, phi_ref)
    both_parities(phi_ref, table_ref, back, back_ref, first)
    decaying_sums(1, gz, decay_ref, scale_ref, phi_ref)
    decaying_sums(2, gz, decay_ref, scale_ref, phi_ref)
    scatter(0, lane, back_ref, out_ref)
    both_parities(phi_ref, table_ref, back, back_ref, rest)
    scatter(1, lane, back_ref, out_ref)
    scatter(2, lane, back_ref, out_ref)


def backward_x(in_ref, table_ref, out_ref, field_ref, flat_ref, sems):
    lane = lax.broadcasted_iota(jnp.int32, (PLANES, LANES), 1)
    turned = []
    for parity in range(2):
        rows = [pl.ds(parity * SLOT * TILES + j, SLOT, stride=TILES) for j in range(TILES)]
        turned.append(jnp.transpose(jnp.concatenate([in_ref[row, :] for row in rows], axis=1)))
    stores = []
    carry = None
    for n, (first, last) in enumerate(zip(BLOCKS, BLOCKS[1:])):
        tops = [z * CHUNK + y for z in range(PLANES) for y in range(first, last, 8)]
        parts = []
        for parity in range(2):
            value = jnp.concatenate([turned[parity][t : t + 8] for t in tops], axis=0)
            parts.append(product(split(value), table_of(table_ref, parity), ((1,), (0,))))
        for side, value in enumerate((parts[0] + parts[1], parts[0] - parts[1])):
            for j in range(2):
                for i, t in enumerate(tops):
                    z, y = divmod(t, CHUNK)
                    rows = pl.ds(z + y * PITCH, 8, stride=PITCH)
                    field_ref[2 * side + j, rows, :] = value[8 * i : 8 * i + 8, lane_tile(j)]
        for piece in range(2 * first, 2 * min(last, ROWS)):
            y, side = divmod(piece, 2)
            offset = piece * HALF
            shift = offset % LANES
            end = shift + HALF
            tiles = [field_ref[2 * side + j, pl.ds(y * PITCH, PLANES), :] for j in range(2)]
            if end > PAIR:
                tiles.append(jnp.zeros((PLANES, LANES), F32))
            tiles = shift_lanes(tiles, shift, lane)
            if carry is not None:
                tiles[0] = tiles[0] + carry
            full = end // LANES
            carry = tiles[full] if end % LANES else None
            for j in range(full):
                flat_ref[:, pl.ds(offset - shift + j * LANES, LANES)] = tiles[j]
        part = pl.ds(first * NX, (min(last, ROWS) - first) * NX)
        stores.append(pltpu.make_async_copy(flat_ref.at[:, part], out_ref.at[:, part], sems.at[n]))
        stores[-1].start()
    for store in stores:
        store.wait()


def exchange(buffer):
    whole = buffer.reshape(PEERS, 1, BELONG * LANES)
    whole = lax.all_to_all(whole, ("core", "gz", "x"), 0, 0, tiled=True)
    return whole.reshape(SEND, LANES)


def on_device(density):
    table_x = jnp.asarray(x_table())
    table_y = jnp.asarray(y_table())
    vmem = pl.BlockSpec(memory_space=pltpu.VMEM)
    hbm = pl.BlockSpec(memory_space=pl.ANY)
    field = pltpu.VMEM((4, CHUNK * PITCH, LANES), F32)
    flat = pltpu.VMEM(density.shape, F32)
    square = pltpu.VMEM((PAD, PAD), F32)
    message = pltpu.VMEM((SEND, LANES), F32)
    groups = pltpu.SemaphoreType.DMA((len(PARTS) - 1,))

    def here(value):
        return pltpu.with_memory_space_constraint(value, pltpu.VMEM)

    factors = pltpu.VMEM((8 * OWN, PAD), F32)
    sent, decay, scale = pl.pallas_call(
        forward_x,
        out_shape=(message, factors, factors),
        in_specs=[hbm, hbm],
        out_specs=(vmem, vmem, vmem),
        scratch_shapes=[
            field,
            flat,
            pltpu.VMEM(table_x.shape, BF16),
            groups,
            pltpu.SemaphoreType.DMA,
        ],
    )(density, table_x)
    back = pl.pallas_call(
        middle,
        out_shape=message,
        in_specs=[vmem, vmem, vmem, vmem],
        out_specs=vmem,
        scratch_shapes=[square, square, square],
    )(here(exchange(sent)), here(table_y), here(decay), here(scale))
    return pl.pallas_call(
        backward_x,
        out_shape=jax.ShapeDtypeStruct(density.shape, F32),
        in_specs=[vmem, vmem],
        out_specs=hbm,
        scratch_shapes=[field, flat, pltpu.SemaphoreType.DMA((len(BLOCKS) - 1,))],
    )(here(exchange(back)), here(table_x))


def solution(mesh):
    split_rows = Mesh(mesh.devices.reshape(GZ, GX, CORES), ("gz", "x", "core"))
    spec = P("gz", ("x", "core"))
    return jax.shard_map(
        on_device,
        mesh=split_rows,
        in_specs=(spec,),
        out_specs=spec,
        check_vma=False,
    )
```

```python
import math

import jax
import jax.numpy as jnp
import numpy as np
from jax import lax
from jax.experimental import pallas as pl
from jax.experimental.pallas import tpu as pltpu
from jax.sharding import Mesh
from jax.sharding import PartitionSpec as P

NX = 352
NY = 352
SCREEN = 128
TWO_PI = 2.0 * math.pi

PAD = 384
LANES = 128
TILES = PAD // LANES
HALF = NX // 2
SLOT = PAD // 2
PAIR = 2 * LANES
GZ = 16
GX = 4
CORES = 2
GY = GX * CORES
PLANES = 8
ROWS = NY // GY
CHUNK = PAD // GY
PITCH = PLANES + 1
BLOCKS = (0, 16, 32, CHUNK)
PARTS = (0, 24, ROWS)
OWN = 3
PEERS = GZ * GY
SEND = PEERS * OWN * TILES
BELONG = OWN * TILES

F32 = jnp.float32
BF16 = jnp.bfloat16


def component(parity, row):
    return 2 * ((row + 1 - parity) >> 1) + parity


def half_basis(length):
    half = length // 2
    index = np.arange(half)
    basis = np.zeros((2, half, half))
    for parity in range(2):
        for row in range(half):
            m = component(parity, row)
            angle = 2.0 * np.pi * ((m * index) % length) / length
            cosine = row == 0 or (row + parity) % 2 == 1 or m == half
            if parity == 1:
                cosine = row % 2 == 0
            weight = 1.0 if m in (0, half) else 2.0
            basis[parity, row] = (np.cos(angle) if cosine else np.sin(angle)) * np.sqrt(weight / length)
    return basis


def halves(table):
    single = table.astype(np.float32)
    high = single.astype(jnp.bfloat16)
    low = (single - high.astype(np.float32)).astype(jnp.bfloat16)
    return np.stack([high, low])


def x_table():
    table = np.zeros((2, SLOT, PAIR))
    table[:, :HALF, :HALF] = half_basis(NX)
    return halves(table)


def x_back_table():
    table = np.zeros((2, PAIR, PAIR))
    basis = half_basis(NX)
    table[0, :HALF, :HALF] = basis[0]
    table[1, PAIR - SLOT : PAIR - SLOT + HALF, :HALF] = basis[1]
    return halves(table)


def y_table():
    block = np.zeros((2, SLOT, GY // 2, CHUNK))
    block[:, :HALF, :, :ROWS] = half_basis(NY).reshape(2, HALF, GY // 2, ROWS)
    block = block.reshape(2, SLOT, SLOT)
    table = np.zeros((2, PAIR, PAIR))
    table[0, :SLOT, :SLOT] = block[0]
    table[1, PAIR - SLOT :, PAIR - SLOT :] = block[1]
    return halves(table)


def split(value):
    high = value.astype(BF16)
    return high, (value - high.astype(F32)).astype(BF16)


def product(left, right, dims):
    def dot(a, b):
        return lax.dot_general(a, b, (dims, ((), ())), preferred_element_type=F32)

    return dot(left[0], right[0]) + (dot(left[0], right[1]) + dot(left[1], right[0]))


def lane_tile(j):
    return slice(j * LANES, (j + 1) * LANES)


def table_of(table_ref, parity):
    return table_ref[0, parity], table_ref[1, parity]


def shift_lanes(tiles, amount, lane):
    count = len(tiles)
    whole, part = divmod(amount % (count * LANES), LANES)
    if part:
        turned = [pltpu.roll(t, part, 1) for t in tiles]
        tiles = [jnp.where(lane < part, turned[j - 1], turned[j]) for j in range(count)]
    return [tiles[(j - whole) % count] for j in range(count)]


def half_row(ref, offset, lane):
    shift = offset % LANES
    count = -(-(shift + HALF) // LANES)
    tiles = [ref[:, pl.ds(offset - shift + j * LANES, LANES)] for j in range(count)]
    return shift_lanes(tiles, -shift, lane)[:2]


def forward_x(x_ref, table_ref, out_ref, decay_ref, scale_ref, field_ref, flat_ref, local_ref, x_sems, table_sem):
    lane = lax.broadcasted_iota(jnp.int32, (PLANES, LANES), 1)
    loads = []
    for n, (first, last) in enumerate(zip(PARTS, PARTS[1:])):
        part = pl.ds(first * NX, (last - first) * NX)
        loads.append(pltpu.make_async_copy(x_ref.at[:, part], flat_ref.at[:, part], x_sems.at[n]))
    table_load = pltpu.make_async_copy(table_ref, local_ref, table_sem)
    for load in loads:
        load.start()
    table_load.start()
    for own in range(OWN):
        for j in range(TILES):
            kappa = kappa_tile(own, j)
            decay_ref[pl.ds(8 * own, 8), lane_tile(j)] = jnp.exp(-kappa)
            scale_ref[pl.ds(8 * own, 8), lane_tile(j)] = 0.5 / kappa
    for y in range(ROWS, CHUNK):
        for j in range(4):
            field_ref[j, pl.ds(y * PITCH, PLANES), :] = jnp.zeros((PLANES, LANES), F32)
    for load, first, last in zip(loads, PARTS, PARTS[1:]):
        load.wait()
        for y in range(first, last):
            one = half_row(flat_ref, y * NX, lane)
            two = half_row(flat_ref, y * NX + HALF, lane)
            for j in range(2):
                field_ref[j, pl.ds(y * PITCH, PLANES), :] = one[j] + two[j]
                field_ref[2 + j, pl.ds(y * PITCH, PLANES), :] = one[j] - two[j]
    table_load.wait()
    for parity in range(2):
        columns = []
        for j in range(2):
            rows = [
                field_ref[2 * parity + j, pl.ds(z + y * PITCH, 8, stride=PITCH), :]
                for z in range(PLANES)
                for y in range(0, CHUNK, 8)
            ]
            columns.append(jnp.concatenate(rows, axis=0))
        field = jnp.concatenate(columns, axis=1)
        result = product(table_of(local_ref, parity), split(field), ((1,), (1,)))
        for j in range(TILES):
            out_ref[pl.ds(parity * SLOT * TILES + j, SLOT, stride=TILES), :] = result[:, lane_tile(j)]


def chunk_pick(parts, lane):
    out = []
    for j in range(TILES):
        first = j * LANES // CHUNK
        last = ((j + 1) * LANES - 1) // CHUNK
        value = parts[last][j]
        for c in range(last - 1, first - 1, -1):
            value = jnp.where(lane < (c + 1) * CHUNK - j * LANES, parts[c][j], value)
        out.append(value)
    return out


def swap_chunks(arrays, lane):
    turned = []
    for d in range(GY):
        picked = chunk_pick([arrays[(c + d) % GY] for c in range(GY)], lane)
        turned.append(shift_lanes(picked, CHUNK * d, lane))
    return [chunk_pick([turned[(c - b) % GY] for c in range(GY)], lane) for b in range(GY)]


def butterfly(arrays):
    pairs = [list(zip(arrays[g], arrays[g + GY // 2])) for g in range(GY // 2)]
    return [[a + b for a, b in p] for p in pairs] + [[a - b for a, b in p] for p in pairs]


def both_parities(value_ref, table_ref, dims, out_ref, rows):
    even = product(split(value_ref[rows, :PAIR]), table_of(table_ref, 0), dims)
    odd = product(split(value_ref[rows, PAD - PAIR :]), table_of(table_ref, 1), dims)
    out_ref[rows, lane_tile(0)] = even[:, :LANES]
    out_ref[rows, lane_tile(1)] = even[:, LANES:] + odd[:, :LANES]
    out_ref[rows, lane_tile(2)] = odd[:, LANES:]


def wavenumber(index, length):
    parity = (index >= SLOT).astype(jnp.int32)
    row = jnp.minimum(index - SLOT * parity, HALF - 1)
    return component(parity, row).astype(F32) * (TWO_PI / length)


def kappa_tile(own, j):
    place = (lax.axis_index("core") * GZ + lax.axis_index("gz")) * GX + lax.axis_index("x")
    index_x = jnp.full((8, LANES), place * OWN + own, jnp.int32)
    index_y = lax.broadcasted_iota(jnp.int32, (8, LANES), 1) + j * LANES
    wave_x = wavenumber(index_x, NX)
    wave_y = wavenumber(index_y, NY)
    return jnp.sqrt(1.0 / (SCREEN * SCREEN) + wave_x * wave_x + wave_y * wave_y)


def message_row(half, g, own, j):
    x, core = divmod(g, CORES)
    first = ((core * GZ + half * 8) * GX + x) * BELONG + own * TILES + j
    return pl.ds(first, 8, stride=GX * BELONG)


def plane_row(own, z, half=0):
    return own * PLANES * GZ + z * GZ + half * 8


def gather(own, lane, in_ref, work_ref):
    for half in range(GZ // 8):
        arrays = [[in_ref[message_row(half, g, own, j), :] for j in range(TILES)] for g in range(GY)]
        for z, parts in enumerate(swap_chunks(butterfly(arrays), lane)):
            for j in range(TILES):
                work_ref[pl.ds(plane_row(own, z, half), 8), lane_tile(j)] = parts[j]


def scatter(own, lane, work_ref, out_ref):
    for half in range(GZ // 8):
        arrays = [
            [work_ref[pl.ds(plane_row(own, z, half), 8), lane_tile(j)] for j in range(TILES)] for z in range(PLANES)
        ]
        for g, parts in enumerate(butterfly(swap_chunks(arrays, lane))):
            for j in range(TILES):
                out_ref[message_row(half, g, own, j), :] = parts[j]


def decaying_sums(own, gz, decay_ref, scale_ref, phi_ref):
    for j in range(TILES):
        decay = decay_ref[pl.ds(8 * own, 8), lane_tile(j)]
        scale = scale_ref[pl.ds(8 * own, 8), lane_tile(j)]
        power = decay * decay
        power = power * power
        power = power * power
        decay, scale, power = (jnp.concatenate([t] * (GZ // 8), axis=0) for t in (decay, scale, power))
        hat = [phi_ref[pl.ds(plane_row(own, z), GZ), lane_tile(j)] for z in range(PLANES)]
        over = hat[0]
        for z in range(1, PLANES):
            over = decay * over + hat[z]
        under = hat[-1]
        for z in range(PLANES - 2, -1, -1):
            under = decay * under + hat[z]
        under = decay * under
        step = 1
        while step < GZ:
            over = over + jnp.where(gz >= step, power * pltpu.roll(over, step, 0), 0.0)
            under = under + jnp.where(gz < GZ - step, power * pltpu.roll(under, GZ - step, 0), 0.0)
            power = power * power
            step *= 2
        over = jnp.where(gz >= 1, pltpu.roll(over, 1, 0), 0.0)
        under = jnp.where(gz < GZ - 1, pltpu.roll(under, GZ - 1, 0), 0.0)
        down = []
        for z in range(PLANES - 1, -1, -1):
            down.append(under)
            under = decay * (under + hat[z])
        for z in range(PLANES):
            over = decay * over + hat[z]
            phi_ref[pl.ds(plane_row(own, z), GZ), lane_tile(j)] = (over + down[PLANES - 1 - z]) * scale


def middle(in_ref, table_ref, decay_ref, scale_ref, out_ref, work_ref, phi_ref, back_ref):
    lane = lax.broadcasted_iota(jnp.int32, (8, LANES), 1)
    gz = lax.broadcasted_iota(jnp.int32, (GZ, LANES), 0)
    forth = ((1,), (1,))
    back = ((1,), (0,))
    every = pl.ds(0, PAD)

    def rows(own):
        return pl.ds(own * PLANES * GZ, PLANES * GZ)

    first = pl.ds(0, PLANES * GZ)
    rest = pl.ds(PLANES * GZ, (OWN - 1) * PLANES * GZ)
    for own in range(OWN):
        gather(own, lane, in_ref, work_ref)
    both_parities(work_ref, table_ref, forth, phi_ref, first)
    both_parities(work_ref, table_ref, forth, phi_ref, rest)
    decaying_sums(0, gz, decay_ref, scale_ref, phi_ref)
    both_parities(phi_ref, table_ref, back, back_ref, first)
    decaying_sums(1, gz, decay_ref, scale_ref, phi_ref)
    decaying_sums(2, gz, decay_ref, scale_ref, phi_ref)
    scatter(0, lane, back_ref, out_ref)
    both_parities(phi_ref, table_ref, back, back_ref, rest)
    scatter(1, lane, back_ref, out_ref)
    scatter(2, lane, back_ref, out_ref)


def backward_x(in_ref, table_ref, out_ref, field_ref, flat_ref, sems):
    lane = lax.broadcasted_iota(jnp.int32, (PLANES, LANES), 1)
    whole = jnp.concatenate([in_ref[pl.ds(j, PAD, stride=TILES), :] for j in range(TILES)], axis=1)
    whole = jnp.transpose(whole)
    turned = [whole[:, :PAIR], whole[:, PAD - PAIR :]]
    stores = []
    carry = None
    for n, (first, last) in enumerate(zip(BLOCKS, BLOCKS[1:])):
        tops = [z * CHUNK + y for z in range(PLANES) for y in range(first, last, 8)]
        parts = []
        for parity in range(2):
            value = jnp.concatenate([turned[parity][t : t + 8] for t in tops], axis=0)
            parts.append(product(split(value), table_of(table_ref, parity), ((1,), (0,))))
        for side, value in enumerate((parts[0] + parts[1], parts[0] - parts[1])):
            for j in range(2):
                for i, t in enumerate(tops):
                    z, y = divmod(t, CHUNK)
                    rows = pl.ds(z + y * PITCH, 8, stride=PITCH)
                    field_ref[2 * side + j, rows, :] = value[8 * i : 8 * i + 8, lane_tile(j)]
        for piece in range(2 * first, 2 * min(last, ROWS)):
            y, side = divmod(piece, 2)
            offset = piece * HALF
            shift = offset % LANES
            end = shift + HALF
            tiles = [field_ref[2 * side + j, pl.ds(y * PITCH, PLANES), :] for j in range(2)]
            if end > PAIR:
                tiles.append(jnp.zeros((PLANES, LANES), F32))
            tiles = shift_lanes(tiles, shift, lane)
            if carry is not None:
                tiles[0] = tiles[0] + carry
            full = end // LANES
            carry = tiles[full] if end % LANES else None
            for j in range(full):
                flat_ref[:, pl.ds(offset - shift + j * LANES, LANES)] = tiles[j]
        part = pl.ds(first * NX, (min(last, ROWS) - first) * NX)
        stores.append(pltpu.make_async_copy(flat_ref.at[:, part], out_ref.at[:, part], sems.at[n]))
        stores[-1].start()
    for store in stores:
        store.wait()


def exchange(buffer):
    whole = buffer.reshape(PEERS, 1, BELONG * LANES)
    whole = lax.all_to_all(whole, ("core", "gz", "x"), 0, 0, tiled=True)
    return whole.reshape(SEND, LANES)


def on_device(density):
    table_x = jnp.asarray(x_table())
    table_y = jnp.asarray(y_table())
    vmem = pl.BlockSpec(memory_space=pltpu.VMEM)
    hbm = pl.BlockSpec(memory_space=pl.ANY)
    field = pltpu.VMEM((4, CHUNK * PITCH, LANES), F32)
    flat = pltpu.VMEM(density.shape, F32)
    square = pltpu.VMEM((PAD, PAD), F32)
    message = pltpu.VMEM((SEND, LANES), F32)
    groups = pltpu.SemaphoreType.DMA((len(PARTS) - 1,))

    def here(value):
        return pltpu.with_memory_space_constraint(value, pltpu.VMEM)

    factors = pltpu.VMEM((8 * OWN, PAD), F32)
    sent, decay, scale = pl.pallas_call(
        forward_x,
        out_shape=(message, factors, factors),
        in_specs=[hbm, hbm],
        out_specs=(vmem, vmem, vmem),
        scratch_shapes=[
            field,
            flat,
            pltpu.VMEM(table_x.shape, BF16),
            groups,
            pltpu.SemaphoreType.DMA,
        ],
    )(density, table_x)
    back = pl.pallas_call(
        middle,
        out_shape=message,
        in_specs=[vmem, vmem, vmem, vmem],
        out_specs=vmem,
        scratch_shapes=[square, square, square],
    )(here(exchange(sent)), here(table_y), here(decay), here(scale))
    return pl.pallas_call(
        backward_x,
        out_shape=jax.ShapeDtypeStruct(density.shape, F32),
        in_specs=[vmem, vmem],
        out_specs=hbm,
        scratch_shapes=[field, flat, pltpu.SemaphoreType.DMA((len(BLOCKS) - 1,))],
    )(here(exchange(back)), here(jnp.asarray(x_back_table())))


def solution(mesh):
    split_rows = Mesh(mesh.devices.reshape(GZ, GX, CORES), ("gz", "x", "core"))
    spec = P("gz", ("x", "core"))
    return jax.shard_map(
        on_device,
        mesh=split_rows,
        in_specs=(spec,),
        out_specs=spec,
        check_vma=False,
    )
```

```python
import math

import jax
import jax.numpy as jnp
import numpy as np
from jax import lax
from jax.experimental import pallas as pl
from jax.experimental.pallas import tpu as pltpu
from jax.sharding import Mesh
from jax.sharding import PartitionSpec as P

NX = 352
NY = 352
SCREEN = 128
TWO_PI = 2.0 * math.pi

PAD = 384
LANES = 128
TILES = PAD // LANES
HALF = NX // 2
SLOT = PAD // 2
PAIR = 2 * LANES
GZ = 16
GX = 4
CORES = 2
GY = GX * CORES
PLANES = 8
ROWS = NY // GY
CHUNK = PAD // GY
PITCH = PLANES + 1
BLOCKS = (0, 16, 32, CHUNK)
PARTS = (0, 24, ROWS)
OWN = 3
PEERS = GZ * GY
SEND = PEERS * OWN * TILES
BELONG = OWN * TILES

F32 = jnp.float32
BF16 = jnp.bfloat16


def component(parity, row):
    return 2 * ((row + 1 - parity) >> 1) + parity


def half_basis(length):
    half = length // 2
    index = np.arange(half)
    basis = np.zeros((2, half, half))
    for parity in range(2):
        for row in range(half):
            m = component(parity, row)
            angle = 2.0 * np.pi * ((m * index) % length) / length
            cosine = row == 0 or (row + parity) % 2 == 1 or m == half
            if parity == 1:
                cosine = row % 2 == 0
            weight = 1.0 if m in (0, half) else 2.0
            basis[parity, row] = (np.cos(angle) if cosine else np.sin(angle)) * np.sqrt(weight / length)
    return basis


def halves(table):
    single = table.astype(np.float32)
    high = single.astype(jnp.bfloat16)
    low = (single - high.astype(np.float32)).astype(jnp.bfloat16)
    return np.stack([high, low])


def x_table():
    table = np.zeros((2, SLOT, PAIR))
    table[:, :HALF, :HALF] = half_basis(NX)
    return halves(table)


def x_back_table():
    table = np.zeros((2, PAIR, PAIR))
    basis = half_basis(NX)
    table[0, :HALF, :HALF] = basis[0]
    table[1, PAIR - SLOT : PAIR - SLOT + HALF, :HALF] = basis[1]
    return halves(table)


def y_table():
    block = np.zeros((2, SLOT, GY // 2, CHUNK))
    block[:, :HALF, :, :ROWS] = half_basis(NY).reshape(2, HALF, GY // 2, ROWS)
    block = block.reshape(2, SLOT, SLOT)
    table = np.zeros((2, PAIR, PAIR))
    table[0, :SLOT, :SLOT] = block[0]
    table[1, PAIR - SLOT :, PAIR - SLOT :] = block[1]
    return halves(table)


def split(value):
    high = value.astype(BF16)
    return high, (value - high.astype(F32)).astype(BF16)


def product(left, right, dims):
    def dot(a, b):
        return lax.dot_general(a, b, (dims, ((), ())), preferred_element_type=F32)

    count = left[0].shape[0]
    both = dot(jnp.concatenate(left, axis=0), right[0])
    return both[:count] + (both[count:] + dot(left[0], right[1]))


def lane_tile(j):
    return slice(j * LANES, (j + 1) * LANES)


def table_of(table_ref, parity):
    return table_ref[0, parity], table_ref[1, parity]


def shift_lanes(tiles, amount, lane):
    count = len(tiles)
    whole, part = divmod(amount % (count * LANES), LANES)
    if part:
        turned = [pltpu.roll(t, part, 1) for t in tiles]
        tiles = [jnp.where(lane < part, turned[j - 1], turned[j]) for j in range(count)]
    return [tiles[(j - whole) % count] for j in range(count)]


def half_row(ref, offset, lane):
    shift = offset % LANES
    count = -(-(shift + HALF) // LANES)
    tiles = [ref[:, pl.ds(offset - shift + j * LANES, LANES)] for j in range(count)]
    return shift_lanes(tiles, -shift, lane)[:2]


def forward_x(x_ref, table_ref, out_ref, decay_ref, scale_ref, field_ref, flat_ref, local_ref, x_sems, table_sem):
    lane = lax.broadcasted_iota(jnp.int32, (PLANES, LANES), 1)
    loads = []
    for n, (first, last) in enumerate(zip(PARTS, PARTS[1:])):
        part = pl.ds(first * NX, (last - first) * NX)
        loads.append(pltpu.make_async_copy(x_ref.at[:, part], flat_ref.at[:, part], x_sems.at[n]))
    table_load = pltpu.make_async_copy(table_ref, local_ref, table_sem)
    for load in loads:
        load.start()
    table_load.start()
    for own in range(OWN):
        for j in range(TILES):
            kappa = kappa_tile(own, j)
            decay_ref[pl.ds(8 * own, 8), lane_tile(j)] = jnp.exp(-kappa)
            scale_ref[pl.ds(8 * own, 8), lane_tile(j)] = 0.5 / kappa
    for y in range(ROWS, CHUNK):
        for j in range(4):
            field_ref[j, pl.ds(y * PITCH, PLANES), :] = jnp.zeros((PLANES, LANES), F32)
    for load, first, last in zip(loads, PARTS, PARTS[1:]):
        load.wait()
        for y in range(first, last):
            one = half_row(flat_ref, y * NX, lane)
            two = half_row(flat_ref, y * NX + HALF, lane)
            for j in range(2):
                field_ref[j, pl.ds(y * PITCH, PLANES), :] = one[j] + two[j]
                field_ref[2 + j, pl.ds(y * PITCH, PLANES), :] = one[j] - two[j]
    table_load.wait()
    for parity in range(2):
        columns = []
        for j in range(2):
            rows = [
                field_ref[2 * parity + j, pl.ds(z + y * PITCH, 8, stride=PITCH), :]
                for z in range(PLANES)
                for y in range(0, CHUNK, 8)
            ]
            columns.append(jnp.concatenate(rows, axis=0))
        field = jnp.concatenate(columns, axis=1)
        result = product(table_of(local_ref, parity), split(field), ((1,), (1,)))
        for j in range(TILES):
            out_ref[pl.ds(parity * SLOT * TILES + j, SLOT, stride=TILES), :] = result[:, lane_tile(j)]


def chunk_pick(parts, lane):
    out = []
    for j in range(TILES):
        first = j * LANES // CHUNK
        last = ((j + 1) * LANES - 1) // CHUNK
        value = parts[last][j]
        for c in range(last - 1, first - 1, -1):
            value = jnp.where(lane < (c + 1) * CHUNK - j * LANES, parts[c][j], value)
        out.append(value)
    return out


def swap_chunks(arrays, lane):
    turned = []
    for d in range(GY):
        picked = chunk_pick([arrays[(c + d) % GY] for c in range(GY)], lane)
        turned.append(shift_lanes(picked, CHUNK * d, lane))
    return [chunk_pick([turned[(c - b) % GY] for c in range(GY)], lane) for b in range(GY)]


def butterfly(arrays):
    pairs = [list(zip(arrays[g], arrays[g + GY // 2])) for g in range(GY // 2)]
    return [[a + b for a, b in p] for p in pairs] + [[a - b for a, b in p] for p in pairs]


def both_parities(value_ref, table_ref, dims, out_ref, rows):
    even = product(split(value_ref[rows, :PAIR]), table_of(table_ref, 0), dims)
    odd = product(split(value_ref[rows, PAD - PAIR :]), table_of(table_ref, 1), dims)
    out_ref[rows, lane_tile(0)] = even[:, :LANES]
    out_ref[rows, lane_tile(1)] = even[:, LANES:] + odd[:, :LANES]
    out_ref[rows, lane_tile(2)] = odd[:, LANES:]


def wavenumber(index, length):
    parity = (index >= SLOT).astype(jnp.int32)
    row = jnp.minimum(index - SLOT * parity, HALF - 1)
    return component(parity, row).astype(F32) * (TWO_PI / length)


def kappa_tile(own, j):
    place = (lax.axis_index("core") * GZ + lax.axis_index("gz")) * GX + lax.axis_index("x")
    index_x = jnp.full((8, LANES), place * OWN + own, jnp.int32)
    index_y = lax.broadcasted_iota(jnp.int32, (8, LANES), 1) + j * LANES
    wave_x = wavenumber(index_x, NX)
    wave_y = wavenumber(index_y, NY)
    return jnp.sqrt(1.0 / (SCREEN * SCREEN) + wave_x * wave_x + wave_y * wave_y)


def message_row(half, g, own, j):
    x, core = divmod(g, CORES)
    first = ((core * GZ + half * 8) * GX + x) * BELONG + own * TILES + j
    return pl.ds(first, 8, stride=GX * BELONG)


def plane_row(own, z, half=0):
    return own * PLANES * GZ + z * GZ + half * 8


def gather(own, lane, in_ref, work_ref):
    for half in range(GZ // 8):
        arrays = [[in_ref[message_row(half, g, own, j), :] for j in range(TILES)] for g in range(GY)]
        for z, parts in enumerate(swap_chunks(butterfly(arrays), lane)):
            for j in range(TILES):
                work_ref[pl.ds(plane_row(own, z, half), 8), lane_tile(j)] = parts[j]


def scatter(own, lane, work_ref, out_ref):
    for half in range(GZ // 8):
        arrays = [
            [work_ref[pl.ds(plane_row(own, z, half), 8), lane_tile(j)] for j in range(TILES)] for z in range(PLANES)
        ]
        for g, parts in enumerate(butterfly(swap_chunks(arrays, lane))):
            for j in range(TILES):
                out_ref[message_row(half, g, own, j), :] = parts[j]


def decaying_sums(own, gz, decay_ref, scale_ref, phi_ref):
    for j in range(TILES):
        decay = decay_ref[pl.ds(8 * own, 8), lane_tile(j)]
        scale = scale_ref[pl.ds(8 * own, 8), lane_tile(j)]
        power = decay * decay
        power = power * power
        power = power * power
        decay, scale, power = (jnp.concatenate([t] * (GZ // 8), axis=0) for t in (decay, scale, power))
        hat = [phi_ref[pl.ds(plane_row(own, z), GZ), lane_tile(j)] for z in range(PLANES)]
        over = hat[0]
        for z in range(1, PLANES):
            over = decay * over + hat[z]
        under = hat[-1]
        for z in range(PLANES - 2, -1, -1):
            under = decay * under + hat[z]
        under = decay * under
        step = 1
        while step < GZ:
            over = over + jnp.where(gz >= step, power * pltpu.roll(over, step, 0), 0.0)
            under = under + jnp.where(gz < GZ - step, power * pltpu.roll(under, GZ - step, 0), 0.0)
            power = power * power
            step *= 2
        over = jnp.where(gz >= 1, pltpu.roll(over, 1, 0), 0.0)
        under = jnp.where(gz < GZ - 1, pltpu.roll(under, GZ - 1, 0), 0.0)
        down = []
        for z in range(PLANES - 1, -1, -1):
            down.append(under)
            under = decay * (under + hat[z])
        for z in range(PLANES):
            over = decay * over + hat[z]
            phi_ref[pl.ds(plane_row(own, z), GZ), lane_tile(j)] = (over + down[PLANES - 1 - z]) * scale


def middle(in_ref, table_ref, decay_ref, scale_ref, out_ref, work_ref, phi_ref, back_ref):
    lane = lax.broadcasted_iota(jnp.int32, (8, LANES), 1)
    gz = lax.broadcasted_iota(jnp.int32, (GZ, LANES), 0)
    forth = ((1,), (1,))
    back = ((1,), (0,))
    every = pl.ds(0, PAD)

    def rows(own):
        return pl.ds(own * PLANES * GZ, PLANES * GZ)

    first = pl.ds(0, PLANES * GZ)
    rest = pl.ds(PLANES * GZ, (OWN - 1) * PLANES * GZ)
    for own in range(OWN):
        gather(own, lane, in_ref, work_ref)
    both_parities(work_ref, table_ref, forth, phi_ref, first)
    both_parities(work_ref, table_ref, forth, phi_ref, rest)
    decaying_sums(0, gz, decay_ref, scale_ref, phi_ref)
    both_parities(phi_ref, table_ref, back, back_ref, first)
    decaying_sums(1, gz, decay_ref, scale_ref, phi_ref)
    decaying_sums(2, gz, decay_ref, scale_ref, phi_ref)
    scatter(0, lane, back_ref, out_ref)
    both_parities(phi_ref, table_ref, back, back_ref, rest)
    scatter(1, lane, back_ref, out_ref)
    scatter(2, lane, back_ref, out_ref)


def backward_x(in_ref, table_ref, out_ref, field_ref, flat_ref, sems):
    lane = lax.broadcasted_iota(jnp.int32, (PLANES, LANES), 1)
    whole = jnp.concatenate([in_ref[pl.ds(j, PAD, stride=TILES), :] for j in range(TILES)], axis=1)
    whole = jnp.transpose(whole)
    turned = [whole[:, :PAIR], whole[:, PAD - PAIR :]]
    stores = []
    carry = None
    for n, (first, last) in enumerate(zip(BLOCKS, BLOCKS[1:])):
        tops = [z * CHUNK + y for z in range(PLANES) for y in range(first, last, 8)]
        parts = []
        for parity in range(2):
            value = jnp.concatenate([turned[parity][t : t + 8] for t in tops], axis=0)
            parts.append(product(split(value), table_of(table_ref, parity), ((1,), (0,))))
        for side, value in enumerate((parts[0] + parts[1], parts[0] - parts[1])):
            for j in range(2):
                for i, t in enumerate(tops):
                    z, y = divmod(t, CHUNK)
                    rows = pl.ds(z + y * PITCH, 8, stride=PITCH)
                    field_ref[2 * side + j, rows, :] = value[8 * i : 8 * i + 8, lane_tile(j)]
        for piece in range(2 * first, 2 * min(last, ROWS)):
            y, side = divmod(piece, 2)
            offset = piece * HALF
            shift = offset % LANES
            end = shift + HALF
            tiles = [field_ref[2 * side + j, pl.ds(y * PITCH, PLANES), :] for j in range(2)]
            if end > PAIR:
                tiles.append(jnp.zeros((PLANES, LANES), F32))
            tiles = shift_lanes(tiles, shift, lane)
            if carry is not None:
                tiles[0] = tiles[0] + carry
            full = end // LANES
            carry = tiles[full] if end % LANES else None
            for j in range(full):
                flat_ref[:, pl.ds(offset - shift + j * LANES, LANES)] = tiles[j]
        part = pl.ds(first * NX, (min(last, ROWS) - first) * NX)
        stores.append(pltpu.make_async_copy(flat_ref.at[:, part], out_ref.at[:, part], sems.at[n]))
        stores[-1].start()
    for store in stores:
        store.wait()


def exchange(buffer):
    whole = buffer.reshape(PEERS, 1, BELONG * LANES)
    whole = lax.all_to_all(whole, ("core", "gz", "x"), 0, 0, tiled=True)
    return whole.reshape(SEND, LANES)


def on_device(density):
    table_x = jnp.asarray(x_table())
    table_y = jnp.asarray(y_table())
    vmem = pl.BlockSpec(memory_space=pltpu.VMEM)
    hbm = pl.BlockSpec(memory_space=pl.ANY)
    field = pltpu.VMEM((4, CHUNK * PITCH, LANES), F32)
    flat = pltpu.VMEM(density.shape, F32)
    square = pltpu.VMEM((PAD, PAD), F32)
    message = pltpu.VMEM((SEND, LANES), F32)
    groups = pltpu.SemaphoreType.DMA((len(PARTS) - 1,))

    def here(value):
        return pltpu.with_memory_space_constraint(value, pltpu.VMEM)

    factors = pltpu.VMEM((8 * OWN, PAD), F32)
    sent, decay, scale = pl.pallas_call(
        forward_x,
        out_shape=(message, factors, factors),
        in_specs=[hbm, hbm],
        out_specs=(vmem, vmem, vmem),
        scratch_shapes=[
            field,
            flat,
            pltpu.VMEM(table_x.shape, BF16),
            groups,
            pltpu.SemaphoreType.DMA,
        ],
    )(density, table_x)
    back = pl.pallas_call(
        middle,
        out_shape=message,
        in_specs=[vmem, vmem, vmem, vmem],
        out_specs=vmem,
        scratch_shapes=[square, square, square],
    )(here(exchange(sent)), here(table_y), here(decay), here(scale))
    return pl.pallas_call(
        backward_x,
        out_shape=jax.ShapeDtypeStruct(density.shape, F32),
        in_specs=[vmem, vmem],
        out_specs=hbm,
        scratch_shapes=[field, flat, pltpu.SemaphoreType.DMA((len(BLOCKS) - 1,))],
    )(here(exchange(back)), here(jnp.asarray(x_back_table())))


def solution(mesh):
    split_rows = Mesh(mesh.devices.reshape(GZ, GX, CORES), ("gz", "x", "core"))
    spec = P("gz", ("x", "core"))
    return jax.shard_map(
        on_device,
        mesh=split_rows,
        in_specs=(spec,),
        out_specs=spec,
        check_vma=False,
    )
```

```python
import math

import jax
import jax.numpy as jnp
import numpy as np
from jax import lax
from jax.experimental import pallas as pl
from jax.experimental.pallas import tpu as pltpu
from jax.sharding import Mesh
from jax.sharding import PartitionSpec as P

NX = 352
NY = 352
SCREEN = 128
TWO_PI = 2.0 * math.pi

PAD = 384
LANES = 128
TILES = PAD // LANES
HALF = NX // 2
SLOT = PAD // 2
PAIR = 2 * LANES
GZ = 16
GX = 4
CORES = 2
GY = GX * CORES
PLANES = 8
ROWS = NY // GY
CHUNK = PAD // GY
PITCH = PLANES + 1
BLOCKS = (0, 16, 32, CHUNK)
PARTS = (0, 24, ROWS)
OWN = 3
PEERS = GZ * GY
SEND = PEERS * OWN * TILES
BELONG = OWN * TILES

F32 = jnp.float32
BF16 = jnp.bfloat16


def component(parity, row):
    return 2 * ((row + 1 - parity) >> 1) + parity


def half_basis(length):
    half = length // 2
    index = np.arange(half)
    basis = np.zeros((2, half, half))
    for parity in range(2):
        for row in range(half):
            m = component(parity, row)
            angle = 2.0 * np.pi * ((m * index) % length) / length
            cosine = row == 0 or (row + parity) % 2 == 1 or m == half
            if parity == 1:
                cosine = row % 2 == 0
            weight = 1.0 if m in (0, half) else 2.0
            basis[parity, row] = (np.cos(angle) if cosine else np.sin(angle)) * np.sqrt(weight / length)
    return basis


def halves(table):
    single = table.astype(np.float32)
    high = single.astype(jnp.bfloat16)
    low = (single - high.astype(np.float32)).astype(jnp.bfloat16)
    return np.stack([high, low])


def x_table():
    table = np.zeros((2, SLOT, PAIR))
    table[:, :HALF, :HALF] = half_basis(NX)
    return halves(table)


def x_back_table():
    table = np.zeros((2, PAIR, PAIR))
    basis = half_basis(NX)
    table[0, :HALF, :HALF] = basis[0]
    table[1, PAIR - SLOT : PAIR - SLOT + HALF, :HALF] = basis[1]
    return halves(table)


def y_table():
    block = np.zeros((2, SLOT, GY // 2, CHUNK))
    block[:, :HALF, :, :ROWS] = half_basis(NY).reshape(2, HALF, GY // 2, ROWS)
    block = block.reshape(2, SLOT, SLOT)
    table = np.zeros((2, PAIR, PAIR))
    table[0, :SLOT, :SLOT] = block[0]
    table[1, PAIR - SLOT :, PAIR - SLOT :] = block[1]
    return halves(table)


def split(value):
    high = value.astype(BF16)
    return high, (value - high.astype(F32)).astype(BF16)


def product(left, right, dims):
    def dot(a, b):
        return lax.dot_general(a, b, (dims, ((), ())), preferred_element_type=F32)

    count = left[0].shape[0]
    both = dot(jnp.concatenate(left, axis=0), right[0])
    return both[:count] + (both[count:] + dot(left[0], right[1]))


def lane_tile(j):
    return slice(j * LANES, (j + 1) * LANES)


def table_of(table_ref, parity):
    return table_ref[0, parity], table_ref[1, parity]


def shift_lanes(tiles, amount, lane):
    count = len(tiles)
    whole, part = divmod(amount % (count * LANES), LANES)
    if part:
        turned = [pltpu.roll(t, part, 1) for t in tiles]
        tiles = [jnp.where(lane < part, turned[j - 1], turned[j]) for j in range(count)]
    return [tiles[(j - whole) % count] for j in range(count)]


def half_row(ref, offset, lane):
    shift = offset % LANES
    count = -(-(shift + HALF) // LANES)
    tiles = [ref[:, pl.ds(offset - shift + j * LANES, LANES)] for j in range(count)]
    return shift_lanes(tiles, -shift, lane)[:2]


def forward_x(x_ref, table_ref, out_ref, decay_ref, scale_ref, field_ref, flat_ref, local_ref, x_sems, table_sem):
    lane = lax.broadcasted_iota(jnp.int32, (PLANES, LANES), 1)
    loads = []
    for n, (first, last) in enumerate(zip(PARTS, PARTS[1:])):
        part = pl.ds(first * NX, (last - first) * NX)
        loads.append(pltpu.make_async_copy(x_ref.at[:, part], flat_ref.at[:, part], x_sems.at[n]))
    table_load = pltpu.make_async_copy(table_ref, local_ref, table_sem)
    for load in loads:
        load.start()
    table_load.start()
    for own in range(OWN):
        for j in range(TILES):
            kappa = kappa_tile(own, j)
            decay_ref[pl.ds(8 * own, 8), lane_tile(j)] = jnp.exp(-kappa)
            scale_ref[pl.ds(8 * own, 8), lane_tile(j)] = 0.5 / kappa
    for y in range(ROWS, CHUNK):
        for j in range(4):
            field_ref[j, pl.ds(y * PITCH, PLANES), :] = jnp.zeros((PLANES, LANES), F32)
    for load, first, last in zip(loads, PARTS, PARTS[1:]):
        load.wait()
        for y in range(first, last):
            one = half_row(flat_ref, y * NX, lane)
            two = half_row(flat_ref, y * NX + HALF, lane)
            for j in range(2):
                field_ref[j, pl.ds(y * PITCH, PLANES), :] = one[j] + two[j]
                field_ref[2 + j, pl.ds(y * PITCH, PLANES), :] = one[j] - two[j]
    table_load.wait()
    for parity in range(2):
        columns = []
        for j in range(2):
            rows = [
                field_ref[2 * parity + j, pl.ds(z + y * PITCH, 8, stride=PITCH), :]
                for z in range(PLANES)
                for y in range(0, CHUNK, 8)
            ]
            columns.append(jnp.concatenate(rows, axis=0))
        field = jnp.concatenate(columns, axis=1)
        result = product(table_of(local_ref, parity), split(field), ((1,), (1,)))
        for j in range(TILES):
            out_ref[pl.ds(parity * SLOT * TILES + j, SLOT, stride=TILES), :] = result[:, lane_tile(j)]


def chunk_pick(parts, lane):
    out = []
    for j in range(TILES):
        first = j * LANES // CHUNK
        last = ((j + 1) * LANES - 1) // CHUNK
        value = parts[last][j]
        for c in range(last - 1, first - 1, -1):
            value = jnp.where(lane < (c + 1) * CHUNK - j * LANES, parts[c][j], value)
        out.append(value)
    return out


def swap_chunks(arrays, lane):
    turned = []
    for d in range(GY):
        picked = chunk_pick([arrays[(c + d) % GY] for c in range(GY)], lane)
        turned.append(shift_lanes(picked, CHUNK * d, lane))
    return [chunk_pick([turned[(c - b) % GY] for c in range(GY)], lane) for b in range(GY)]


def butterfly(arrays):
    pairs = [list(zip(arrays[g], arrays[g + GY // 2])) for g in range(GY // 2)]
    return [[a + b for a, b in p] for p in pairs] + [[a - b for a, b in p] for p in pairs]


def both_parities(value_ref, table_ref, dims, out_ref, rows):
    even = product(split(value_ref[rows, :PAIR]), table_of(table_ref, 0), dims)
    odd = product(split(value_ref[rows, PAD - PAIR :]), table_of(table_ref, 1), dims)
    out_ref[rows, lane_tile(0)] = even[:, :LANES]
    out_ref[rows, lane_tile(1)] = even[:, LANES:] + odd[:, :LANES]
    out_ref[rows, lane_tile(2)] = odd[:, LANES:]


def wavenumber(index, length):
    parity = (index >= SLOT).astype(jnp.int32)
    row = jnp.minimum(index - SLOT * parity, HALF - 1)
    return component(parity, row).astype(F32) * (TWO_PI / length)


def kappa_tile(own, j):
    place = (lax.axis_index("core") * GZ + lax.axis_index("gz")) * GX + lax.axis_index("x")
    index_x = jnp.full((8, LANES), place * OWN + own, jnp.int32)
    index_y = lax.broadcasted_iota(jnp.int32, (8, LANES), 1) + j * LANES
    wave_x = wavenumber(index_x, NX)
    wave_y = wavenumber(index_y, NY)
    return jnp.sqrt(1.0 / (SCREEN * SCREEN) + wave_x * wave_x + wave_y * wave_y)


def message_row(half, g, own, j):
    x, core = divmod(g, CORES)
    first = ((core * GZ + half * 8) * GX + x) * BELONG + own * TILES + j
    return pl.ds(first, 8, stride=GX * BELONG)


def plane_row(own, z, half=0):
    return own * PLANES * GZ + z * GZ + half * 8


def gather(own, lane, in_ref, work_ref):
    for half in range(GZ // 8):
        arrays = [[in_ref[message_row(half, g, own, j), :] for j in range(TILES)] for g in range(GY)]
        for z, parts in enumerate(swap_chunks(butterfly(arrays), lane)):
            for j in range(TILES):
                work_ref[pl.ds(plane_row(own, z, half), 8), lane_tile(j)] = parts[j]


def scatter(own, lane, work_ref, out_ref):
    for half in range(GZ // 8):
        arrays = [
            [work_ref[pl.ds(plane_row(own, z, half), 8), lane_tile(j)] for j in range(TILES)] for z in range(PLANES)
        ]
        for g, parts in enumerate(butterfly(swap_chunks(arrays, lane))):
            for j in range(TILES):
                out_ref[message_row(half, g, own, j), :] = parts[j]


def decaying_sums(own, gz, decay_ref, scale_ref, phi_ref):
    for j in range(TILES):
        decay = decay_ref[pl.ds(8 * own, 8), lane_tile(j)]
        scale = scale_ref[pl.ds(8 * own, 8), lane_tile(j)]
        power = decay * decay
        power = power * power
        power = power * power
        decay, scale, power = (jnp.concatenate([t] * (GZ // 8), axis=0) for t in (decay, scale, power))
        hat = [phi_ref[pl.ds(plane_row(own, z), GZ), lane_tile(j)] for z in range(PLANES)]
        over = hat[0]
        for z in range(1, PLANES):
            over = decay * over + hat[z]
        under = hat[-1]
        for z in range(PLANES - 2, -1, -1):
            under = decay * under + hat[z]
        under = decay * under
        step = 1
        while step < GZ:
            over = over + jnp.where(gz >= step, power * pltpu.roll(over, step, 0), 0.0)
            under = under + jnp.where(gz < GZ - step, power * pltpu.roll(under, GZ - step, 0), 0.0)
            power = power * power
            step *= 2
        over = jnp.where(gz >= 1, pltpu.roll(over, 1, 0), 0.0)
        under = jnp.where(gz < GZ - 1, pltpu.roll(under, GZ - 1, 0), 0.0)
        down = []
        for z in range(PLANES - 1, -1, -1):
            down.append(under)
            under = decay * (under + hat[z])
        for z in range(PLANES):
            over = decay * over + hat[z]
            phi_ref[pl.ds(plane_row(own, z), GZ), lane_tile(j)] = (over + down[PLANES - 1 - z]) * scale


def middle(in_ref, turned_ref, table_ref, decay_ref, scale_ref, out_ref, work_ref, phi_ref, back_ref):
    lane = lax.broadcasted_iota(jnp.int32, (8, LANES), 1)
    gz = lax.broadcasted_iota(jnp.int32, (GZ, LANES), 0)
    back = ((1,), (0,))
    every = pl.ds(0, PAD)

    def rows(own):
        return pl.ds(own * PLANES * GZ, PLANES * GZ)

    first = pl.ds(0, PLANES * GZ)
    rest = pl.ds(PLANES * GZ, (OWN - 1) * PLANES * GZ)
    for own in range(OWN):
        gather(own, lane, in_ref, work_ref)
    both_parities(work_ref, turned_ref, back, phi_ref, first)
    both_parities(work_ref, turned_ref, back, phi_ref, rest)
    decaying_sums(0, gz, decay_ref, scale_ref, phi_ref)
    both_parities(phi_ref, table_ref, back, back_ref, first)
    decaying_sums(1, gz, decay_ref, scale_ref, phi_ref)
    decaying_sums(2, gz, decay_ref, scale_ref, phi_ref)
    scatter(0, lane, back_ref, out_ref)
    both_parities(phi_ref, table_ref, back, back_ref, rest)
    scatter(1, lane, back_ref, out_ref)
    scatter(2, lane, back_ref, out_ref)


def backward_x(in_ref, table_ref, out_ref, field_ref, flat_ref, sems):
    lane = lax.broadcasted_iota(jnp.int32, (PLANES, LANES), 1)
    whole = jnp.concatenate([in_ref[pl.ds(j, PAD, stride=TILES), :] for j in range(TILES)], axis=1)
    whole = jnp.transpose(whole)
    turned = [whole[:, :PAIR], whole[:, PAD - PAIR :]]
    stores = []
    carry = None
    for n, (first, last) in enumerate(zip(BLOCKS, BLOCKS[1:])):
        tops = [z * CHUNK + y for z in range(PLANES) for y in range(first, last, 8)]
        parts = []
        for parity in range(2):
            value = jnp.concatenate([turned[parity][t : t + 8] for t in tops], axis=0)
            parts.append(product(split(value), table_of(table_ref, parity), ((1,), (0,))))
        for side, value in enumerate((parts[0] + parts[1], parts[0] - parts[1])):
            for j in range(2):
                for i, t in enumerate(tops):
                    z, y = divmod(t, CHUNK)
                    rows = pl.ds(z + y * PITCH, 8, stride=PITCH)
                    field_ref[2 * side + j, rows, :] = value[8 * i : 8 * i + 8, lane_tile(j)]
        for piece in range(2 * first, 2 * min(last, ROWS)):
            y, side = divmod(piece, 2)
            offset = piece * HALF
            shift = offset % LANES
            end = shift + HALF
            tiles = [field_ref[2 * side + j, pl.ds(y * PITCH, PLANES), :] for j in range(2)]
            if end > PAIR:
                tiles.append(jnp.zeros((PLANES, LANES), F32))
            tiles = shift_lanes(tiles, shift, lane)
            if carry is not None:
                tiles[0] = tiles[0] + carry
            full = end // LANES
            carry = tiles[full] if end % LANES else None
            for j in range(full):
                flat_ref[:, pl.ds(offset - shift + j * LANES, LANES)] = tiles[j]
        part = pl.ds(first * NX, (min(last, ROWS) - first) * NX)
        stores.append(pltpu.make_async_copy(flat_ref.at[:, part], out_ref.at[:, part], sems.at[n]))
        stores[-1].start()
    for store in stores:
        store.wait()


def exchange(buffer):
    whole = buffer.reshape(PEERS, 1, BELONG * LANES)
    whole = lax.all_to_all(whole, ("core", "gz", "x"), 0, 0, tiled=True)
    return whole.reshape(SEND, LANES)


def on_device(density):
    table_x = jnp.asarray(x_table())
    table_y = jnp.asarray(y_table())
    vmem = pl.BlockSpec(memory_space=pltpu.VMEM)
    hbm = pl.BlockSpec(memory_space=pl.ANY)
    field = pltpu.VMEM((4, CHUNK * PITCH, LANES), F32)
    flat = pltpu.VMEM(density.shape, F32)
    square = pltpu.VMEM((PAD, PAD), F32)
    message = pltpu.VMEM((SEND, LANES), F32)
    groups = pltpu.SemaphoreType.DMA((len(PARTS) - 1,))

    def here(value):
        return pltpu.with_memory_space_constraint(value, pltpu.VMEM)

    factors = pltpu.VMEM((8 * OWN, PAD), F32)
    sent, decay, scale = pl.pallas_call(
        forward_x,
        out_shape=(message, factors, factors),
        in_specs=[hbm, hbm],
        out_specs=(vmem, vmem, vmem),
        scratch_shapes=[
            field,
            flat,
            pltpu.VMEM(table_x.shape, BF16),
            groups,
            pltpu.SemaphoreType.DMA,
        ],
    )(density, table_x)
    back = pl.pallas_call(
        middle,
        out_shape=message,
        in_specs=[vmem] * 5,
        out_specs=vmem,
        scratch_shapes=[square, square, square],
    )(here(exchange(sent)), here(jnp.asarray(np.swapaxes(y_table(), 2, 3))), here(table_y), here(decay), here(scale))
    return pl.pallas_call(
        backward_x,
        out_shape=jax.ShapeDtypeStruct(density.shape, F32),
        in_specs=[vmem, vmem],
        out_specs=hbm,
        scratch_shapes=[field, flat, pltpu.SemaphoreType.DMA((len(BLOCKS) - 1,))],
    )(here(exchange(back)), here(jnp.asarray(x_back_table())))


def solution(mesh):
    split_rows = Mesh(mesh.devices.reshape(GZ, GX, CORES), ("gz", "x", "core"))
    spec = P("gz", ("x", "core"))
    return jax.shard_map(
        on_device,
        mesh=split_rows,
        in_specs=(spec,),
        out_specs=spec,
        check_vma=False,
    )
```

```python
import math

import jax
import jax.numpy as jnp
import numpy as np
from jax import lax
from jax.experimental import pallas as pl
from jax.experimental.pallas import tpu as pltpu
from jax.sharding import Mesh
from jax.sharding import PartitionSpec as P

NX = 352
NY = 352
SCREEN = 128
TWO_PI = 2.0 * math.pi

PAD = 384
LANES = 128
TILES = PAD // LANES
HALF = NX // 2
SLOT = PAD // 2
PAIR = 2 * LANES
GZ = 16
GX = 4
CORES = 2
GY = GX * CORES
PLANES = 8
ROWS = NY // GY
CHUNK = PAD // GY
PITCH = PLANES + 1
BLOCKS = (0, 16, 32, CHUNK)
PARTS = (0, ROWS)
OWN = 3
PEERS = GZ * GY
SEND = PEERS * OWN * TILES
BELONG = OWN * TILES

F32 = jnp.float32
BF16 = jnp.bfloat16


def component(parity, row):
    return 2 * ((row + 1 - parity) >> 1) + parity


def half_basis(length):
    half = length // 2
    index = np.arange(half)
    basis = np.zeros((2, half, half))
    for parity in range(2):
        for row in range(half):
            m = component(parity, row)
            angle = 2.0 * np.pi * ((m * index) % length) / length
            cosine = row == 0 or (row + parity) % 2 == 1 or m == half
            if parity == 1:
                cosine = row % 2 == 0
            weight = 1.0 if m in (0, half) else 2.0
            basis[parity, row] = (np.cos(angle) if cosine else np.sin(angle)) * np.sqrt(weight / length)
    return basis


def halves(table):
    single = table.astype(np.float32)
    high = single.astype(jnp.bfloat16)
    low = (single - high.astype(np.float32)).astype(jnp.bfloat16)
    return np.stack([high, low])


def x_table():
    table = np.zeros((2, SLOT, PAIR))
    table[:, :HALF, :HALF] = half_basis(NX)
    return halves(table)


def x_back_table():
    table = np.zeros((2, PAIR, PAIR))
    basis = half_basis(NX)
    table[0, :HALF, :HALF] = basis[0]
    table[1, PAIR - SLOT : PAIR - SLOT + HALF, :HALF] = basis[1]
    return halves(table)


def y_table():
    block = np.zeros((2, SLOT, GY // 2, CHUNK))
    block[:, :HALF, :, :ROWS] = half_basis(NY).reshape(2, HALF, GY // 2, ROWS)
    block = block.reshape(2, SLOT, SLOT)
    table = np.zeros((2, PAIR, PAIR))
    table[0, :SLOT, :SLOT] = block[0]
    table[1, PAIR - SLOT :, PAIR - SLOT :] = block[1]
    return halves(table)


def split(value):
    high = value.astype(BF16)
    return high, (value - high.astype(F32)).astype(BF16)


def product(left, right, dims):
    def dot(a, b):
        return lax.dot_general(a, b, (dims, ((), ())), preferred_element_type=F32)

    count = left[0].shape[0]
    both = dot(jnp.concatenate(left, axis=0), right[0])
    return both[:count] + (both[count:] + dot(left[0], right[1]))


def lane_tile(j):
    return slice(j * LANES, (j + 1) * LANES)


def table_of(table_ref, parity):
    return table_ref[0, parity], table_ref[1, parity]


def shift_lanes(tiles, amount, lane):
    count = len(tiles)
    whole, part = divmod(amount % (count * LANES), LANES)
    if part:
        turned = [pltpu.roll(t, part, 1) for t in tiles]
        tiles = [jnp.where(lane < part, turned[j - 1], turned[j]) for j in range(count)]
    return [tiles[(j - whole) % count] for j in range(count)]


def half_row(ref, offset, lane):
    shift = offset % LANES
    count = -(-(shift + HALF) // LANES)
    tiles = [ref[:, pl.ds(offset - shift + j * LANES, LANES)] for j in range(count)]
    return shift_lanes(tiles, -shift, lane)[:2]


def forward_x(x_ref, table_ref, out_ref, decay_ref, scale_ref, field_ref, flat_ref, local_ref, x_sems, table_sem):
    lane = lax.broadcasted_iota(jnp.int32, (PLANES, LANES), 1)
    loads = []
    for n, (first, last) in enumerate(zip(PARTS, PARTS[1:])):
        part = pl.ds(first * NX, (last - first) * NX)
        loads.append(pltpu.make_async_copy(x_ref.at[:, part], flat_ref.at[:, part], x_sems.at[n]))
    table_load = pltpu.make_async_copy(table_ref, local_ref, table_sem)
    for load in loads:
        load.start()
    table_load.start()
    for own in range(OWN):
        for j in range(TILES):
            kappa = kappa_tile(own, j)
            decay_ref[pl.ds(8 * own, 8), lane_tile(j)] = jnp.exp(-kappa)
            scale_ref[pl.ds(8 * own, 8), lane_tile(j)] = 0.5 / kappa
    for y in range(ROWS, CHUNK):
        for j in range(4):
            field_ref[j, pl.ds(y * PITCH, PLANES), :] = jnp.zeros((PLANES, LANES), F32)
    for load, first, last in zip(loads, PARTS, PARTS[1:]):
        load.wait()
        for y in range(first, last):
            one = half_row(flat_ref, y * NX, lane)
            two = half_row(flat_ref, y * NX + HALF, lane)
            for j in range(2):
                field_ref[j, pl.ds(y * PITCH, PLANES), :] = one[j] + two[j]
                field_ref[2 + j, pl.ds(y * PITCH, PLANES), :] = one[j] - two[j]
    table_load.wait()
    for parity in range(2):
        columns = []
        for j in range(2):
            rows = [
                field_ref[2 * parity + j, pl.ds(z + y * PITCH, 8, stride=PITCH), :]
                for z in range(PLANES)
                for y in range(0, CHUNK, 8)
            ]
            columns.append(jnp.concatenate(rows, axis=0))
        field = jnp.concatenate(columns, axis=1)
        result = product(table_of(local_ref, parity), split(field), ((1,), (1,)))
        for j in range(TILES):
            out_ref[pl.ds(parity * SLOT * TILES + j, SLOT, stride=TILES), :] = result[:, lane_tile(j)]


def chunk_pick(parts, lane):
    out = []
    for j in range(TILES):
        first = j * LANES // CHUNK
        last = ((j + 1) * LANES - 1) // CHUNK
        value = parts[last][j]
        for c in range(last - 1, first - 1, -1):
            value = jnp.where(lane < (c + 1) * CHUNK - j * LANES, parts[c][j], value)
        out.append(value)
    return out


def swap_chunks(arrays, lane):
    turned = []
    for d in range(GY):
        picked = chunk_pick([arrays[(c + d) % GY] for c in range(GY)], lane)
        turned.append(shift_lanes(picked, CHUNK * d, lane))
    return [chunk_pick([turned[(c - b) % GY] for c in range(GY)], lane) for b in range(GY)]


def butterfly(arrays):
    pairs = [list(zip(arrays[g], arrays[g + GY // 2])) for g in range(GY // 2)]
    return [[a + b for a, b in p] for p in pairs] + [[a - b for a, b in p] for p in pairs]


def both_parities(value_ref, table_ref, dims, out_ref, rows):
    even = product(split(value_ref[rows, :PAIR]), table_of(table_ref, 0), dims)
    odd = product(split(value_ref[rows, PAD - PAIR :]), table_of(table_ref, 1), dims)
    out_ref[rows, lane_tile(0)] = even[:, :LANES]
    out_ref[rows, lane_tile(1)] = even[:, LANES:] + odd[:, :LANES]
    out_ref[rows, lane_tile(2)] = odd[:, LANES:]


def wavenumber(index, length):
    parity = (index >= SLOT).astype(jnp.int32)
    row = jnp.minimum(index - SLOT * parity, HALF - 1)
    return component(parity, row).astype(F32) * (TWO_PI / length)


def kappa_tile(own, j):
    place = (lax.axis_index("core") * GZ + lax.axis_index("gz")) * GX + lax.axis_index("x")
    index_x = jnp.full((8, LANES), place * OWN + own, jnp.int32)
    index_y = lax.broadcasted_iota(jnp.int32, (8, LANES), 1) + j * LANES
    wave_x = wavenumber(index_x, NX)
    wave_y = wavenumber(index_y, NY)
    return jnp.sqrt(1.0 / (SCREEN * SCREEN) + wave_x * wave_x + wave_y * wave_y)


def message_row(half, g, own, j):
    x, core = divmod(g, CORES)
    first = ((core * GZ + half * 8) * GX + x) * BELONG + own * TILES + j
    return pl.ds(first, 8, stride=GX * BELONG)


def plane_row(own, z, half=0):
    return own * PLANES * GZ + z * GZ + half * 8


def gather(own, lane, in_ref, work_ref):
    for half in range(GZ // 8):
        arrays = [[in_ref[message_row(half, g, own, j), :] for j in range(TILES)] for g in range(GY)]
        for z, parts in enumerate(swap_chunks(butterfly(arrays), lane)):
            for j in range(TILES):
                work_ref[pl.ds(plane_row(own, z, half), 8), lane_tile(j)] = parts[j]


def scatter(own, lane, work_ref, out_ref):
    for half in range(GZ // 8):
        arrays = [
            [work_ref[pl.ds(plane_row(own, z, half), 8), lane_tile(j)] for j in range(TILES)] for z in range(PLANES)
        ]
        for g, parts in enumerate(butterfly(swap_chunks(arrays, lane))):
            for j in range(TILES):
                out_ref[message_row(half, g, own, j), :] = parts[j]


def decaying_sums(own, gz, decay_ref, scale_ref, phi_ref):
    for j in range(TILES):
        decay = decay_ref[pl.ds(8 * own, 8), lane_tile(j)]
        scale = scale_ref[pl.ds(8 * own, 8), lane_tile(j)]
        power = decay * decay
        power = power * power
        power = power * power
        decay, scale, power = (jnp.concatenate([t] * (GZ // 8), axis=0) for t in (decay, scale, power))
        hat = [phi_ref[pl.ds(plane_row(own, z), GZ), lane_tile(j)] for z in range(PLANES)]
        over = hat[0]
        for z in range(1, PLANES):
            over = decay * over + hat[z]
        under = hat[-1]
        for z in range(PLANES - 2, -1, -1):
            under = decay * under + hat[z]
        under = decay * under
        step = 1
        while step < GZ:
            over = over + jnp.where(gz >= step, power * pltpu.roll(over, step, 0), 0.0)
            under = under + jnp.where(gz < GZ - step, power * pltpu.roll(under, GZ - step, 0), 0.0)
            power = power * power
            step *= 2
        over = jnp.where(gz >= 1, pltpu.roll(over, 1, 0), 0.0)
        under = jnp.where(gz < GZ - 1, pltpu.roll(under, GZ - 1, 0), 0.0)
        down = []
        for z in range(PLANES - 1, -1, -1):
            down.append(under)
            under = decay * (under + hat[z])
        for z in range(PLANES):
            over = decay * over + hat[z]
            phi_ref[pl.ds(plane_row(own, z), GZ), lane_tile(j)] = (over + down[PLANES - 1 - z]) * scale


def middle(in_ref, turned_ref, table_ref, decay_ref, scale_ref, out_ref, work_ref, phi_ref, back_ref):
    lane = lax.broadcasted_iota(jnp.int32, (8, LANES), 1)
    gz = lax.broadcasted_iota(jnp.int32, (GZ, LANES), 0)
    back = ((1,), (0,))
    every = pl.ds(0, PAD)

    def rows(own):
        return pl.ds(own * PLANES * GZ, PLANES * GZ)

    first = pl.ds(0, PLANES * GZ)
    rest = pl.ds(PLANES * GZ, (OWN - 1) * PLANES * GZ)
    for own in range(OWN):
        gather(own, lane, in_ref, work_ref)
    both_parities(work_ref, turned_ref, back, phi_ref, first)
    both_parities(work_ref, turned_ref, back, phi_ref, rest)
    decaying_sums(0, gz, decay_ref, scale_ref, phi_ref)
    both_parities(phi_ref, table_ref, back, back_ref, first)
    decaying_sums(1, gz, decay_ref, scale_ref, phi_ref)
    decaying_sums(2, gz, decay_ref, scale_ref, phi_ref)
    scatter(0, lane, back_ref, out_ref)
    both_parities(phi_ref, table_ref, back, back_ref, rest)
    scatter(1, lane, back_ref, out_ref)
    scatter(2, lane, back_ref, out_ref)


def backward_x(in_ref, table_ref, out_ref, field_ref, flat_ref, sems):
    lane = lax.broadcasted_iota(jnp.int32, (PLANES, LANES), 1)
    whole = jnp.concatenate([in_ref[pl.ds(j, PAD, stride=TILES), :] for j in range(TILES)], axis=1)
    whole = jnp.transpose(whole)
    turned = [whole[:, :PAIR], whole[:, PAD - PAIR :]]
    stores = []
    carry = None
    for n, (first, last) in enumerate(zip(BLOCKS, BLOCKS[1:])):
        tops = [z * CHUNK + y for z in range(PLANES) for y in range(first, last, 8)]
        parts = []
        for parity in range(2):
            value = jnp.concatenate([turned[parity][t : t + 8] for t in tops], axis=0)
            parts.append(product(split(value), table_of(table_ref, parity), ((1,), (0,))))
        for side, value in enumerate((parts[0] + parts[1], parts[0] - parts[1])):
            for j in range(2):
                for i, t in enumerate(tops):
                    z, y = divmod(t, CHUNK)
                    rows = pl.ds(z + y * PITCH, 8, stride=PITCH)
                    field_ref[2 * side + j, rows, :] = value[8 * i : 8 * i + 8, lane_tile(j)]
        for piece in range(2 * first, 2 * min(last, ROWS)):
            y, side = divmod(piece, 2)
            offset = piece * HALF
            shift = offset % LANES
            end = shift + HALF
            tiles = [field_ref[2 * side + j, pl.ds(y * PITCH, PLANES), :] for j in range(2)]
            if end > PAIR:
                tiles.append(jnp.zeros((PLANES, LANES), F32))
            tiles = shift_lanes(tiles, shift, lane)
            if carry is not None:
                tiles[0] = tiles[0] + carry
            full = end // LANES
            carry = tiles[full] if end % LANES else None
            for j in range(full):
                flat_ref[:, pl.ds(offset - shift + j * LANES, LANES)] = tiles[j]
        part = pl.ds(first * NX, (min(last, ROWS) - first) * NX)
        stores.append(pltpu.make_async_copy(flat_ref.at[:, part], out_ref.at[:, part], sems.at[n]))
        stores[-1].start()
    for store in stores:
        store.wait()


def exchange(buffer):
    whole = buffer.reshape(PEERS, 1, BELONG * LANES)
    whole = lax.all_to_all(whole, ("core", "gz", "x"), 0, 0, tiled=True)
    return whole.reshape(SEND, LANES)


def on_device(density):
    table_x = jnp.asarray(x_table())
    table_y = jnp.asarray(y_table())
    vmem = pl.BlockSpec(memory_space=pltpu.VMEM)
    hbm = pl.BlockSpec(memory_space=pl.ANY)
    field = pltpu.VMEM((4, CHUNK * PITCH, LANES), F32)
    flat = pltpu.VMEM(density.shape, F32)
    square = pltpu.VMEM((PAD, PAD), F32)
    message = pltpu.VMEM((SEND, LANES), F32)
    groups = pltpu.SemaphoreType.DMA((len(PARTS) - 1,))

    def here(value):
        return pltpu.with_memory_space_constraint(value, pltpu.VMEM)

    factors = pltpu.VMEM((8 * OWN, PAD), F32)
    sent, decay, scale = pl.pallas_call(
        forward_x,
        out_shape=(message, factors, factors),
        in_specs=[hbm, hbm],
        out_specs=(vmem, vmem, vmem),
        scratch_shapes=[
            field,
            flat,
            pltpu.VMEM(table_x.shape, BF16),
            groups,
            pltpu.SemaphoreType.DMA,
        ],
    )(density, table_x)
    back = pl.pallas_call(
        middle,
        out_shape=message,
        in_specs=[vmem] * 5,
        out_specs=vmem,
        scratch_shapes=[square, square, square],
    )(here(exchange(sent)), here(jnp.asarray(np.swapaxes(y_table(), 2, 3))), here(table_y), here(decay), here(scale))
    return pl.pallas_call(
        backward_x,
        out_shape=jax.ShapeDtypeStruct(density.shape, F32),
        in_specs=[vmem, vmem],
        out_specs=hbm,
        scratch_shapes=[field, flat, pltpu.SemaphoreType.DMA((len(BLOCKS) - 1,))],
    )(here(exchange(back)), here(jnp.asarray(x_back_table())))


def solution(mesh):
    split_rows = Mesh(mesh.devices.reshape(GZ, GX, CORES), ("gz", "x", "core"))
    spec = P("gz", ("x", "core"))
    return jax.shard_map(
        on_device,
        mesh=split_rows,
        in_specs=(spec,),
        out_specs=spec,
        check_vma=False,
    )
```
